32 devices in a mesh: dp: 1 (over z), cp: 32 (over y, x, core).
Axes of the slice: x: 4, y: 4, z: 1, core: 2. Of those that a mesh axis runs over, the one named last changes fastest.
The devices are a block of a 4x4x8 slice.
Arguments:
- x_seq: bfloat16 [1, 8192, 768], P('dp', 'cp')
- dy_seq: float32 [1, 8192, 768], P('dp', 'cp')
- ln1_gain: float32 [768], replicated
- ln1_bias: float32 [768], replicated
- ln2_gain: float32 [768], replicated
- ln2_bias: float32 [768], replicated
- w_qkv: bfloat16 [768, 12, 3, 64], replicated
- b_qkv: bfloat16 [12, 3, 64], replicated
- w_out: bfloat16 [768, 768], replicated
- b_out: bfloat16 [768], replicated
- w_up: bfloat16 [768, 3072], replicated
- b_up: bfloat16 [3072], replicated
- w_down: bfloat16 [3072, 768], replicated
- b_down: bfloat16 [768], replicated
Outputs:
- output 1: bfloat16 [1, 8192, 768], P('dp', 'cp')
- output 2: float32 [1, 8192, 768], P('dp', 'cp')
- output 3: float32 [768], P('dp')
- output 4: float32 [768], P('dp')
- output 5: float32 [768], P('dp')
- output 6: float32 [768], P('dp')
- output 7: float32 [768, 12, 3, 64], P('dp')
- output 8: float32 [12, 3, 64], P('dp')
- output 9: float32 [768, 768], P('dp')
- output 10: float32 [768], P('dp')
- output 11: float32 [768, 3072], P('dp')
- output 12: float32 [3072], P('dp')
- output 13: float32 [3072, 768], P('dp')
- output 14: float32 [768], P('dp')
All inputs are finite; a program needn't handle non-finite values.
Results may differ from the reference program's by a relative error of at most 0.0195307.
Values are sent between devices in bfloat16 or wider.
A program may use at most 768 MiB of HBM per device.

```python
import math
import jax
import jax.numpy as jnp
from jax import lax

D = 768
HEADS = 12
HEAD = 64
FF = 3072
BATCH = 1
SEQ = 8192
ROT = HEAD // 4
QBLK = min(SEQ, 128)
EPS = 1e-5
ROPE_BASE = 10000.0
NEG_BIG = -1e30


def setup_inputs(seed: int = 0, part: int = 0) -> dict:
    part_key = jax.random.fold_in(jax.random.key(seed), part)
    act_keys = jax.random.split(part_key, 2)
    weight_keys = jax.random.split(jax.random.key(seed + 1), 12)
    qk_gain = max(math.log(SEQ / 16.0), 1.0) ** 0.25
    col_scale = jnp.array([qk_gain, qk_gain, 1.0], dtype=jnp.float32)[None, None, :, None] * D ** -0.5

    def normal(rand_key, arr_shape):
        return jax.random.normal(rand_key, arr_shape, dtype=jnp.float32)

    return {
        'x_seq': normal(act_keys[0], (BATCH, SEQ, D)).astype(jnp.bfloat16),
        'dy_seq': normal(act_keys[1], (BATCH, SEQ, D)),
        'ln1_gain': 1.0 + 0.3 * normal(weight_keys[0], (D,)),
        'ln1_bias': 0.3 * normal(weight_keys[1], (D,)),
        'ln2_gain': 1.0 + 0.3 * normal(weight_keys[2], (D,)),
        'ln2_bias': 0.3 * normal(weight_keys[3], (D,)),
        'w_qkv': (normal(weight_keys[4], (D, HEADS, 3, HEAD)) * col_scale).astype(jnp.bfloat16),
        'b_qkv': (0.3 * normal(weight_keys[5], (HEADS, 3, HEAD))).astype(jnp.bfloat16),
        'w_out': (2.0 * D ** -0.5 * normal(weight_keys[6], (D, D))).astype(jnp.bfloat16),
        'b_out': (0.3 * normal(weight_keys[7], (D,))).astype(jnp.bfloat16),
        'w_up': (D ** -0.5 * normal(weight_keys[8], (D, FF))).astype(jnp.bfloat16),
        'b_up': (0.3 * normal(weight_keys[9], (FF,))).astype(jnp.bfloat16),
        'w_down': (FF ** -0.5 * normal(weight_keys[10], (FF, D))).astype(jnp.bfloat16),
        'b_down': (0.3 * normal(weight_keys[11], (D,))).astype(jnp.bfloat16),
    }


def as_stored(values_in):
    return values_in + lax.stop_gradient(values_in.astype(jnp.bfloat16).astype(jnp.float32) - values_in)


def layer_norm(row_vals, norm_gain, norm_shift):
    row_mean = jnp.mean(row_vals, axis=-1, keepdims=True)
    centered = row_vals - row_mean
    row_var = jnp.mean(centered * centered, axis=-1, keepdims=True)
    return centered * lax.rsqrt(row_var + EPS) * norm_gain + norm_shift


def rope_tables():
    inv_freq = ROPE_BASE ** (-jnp.arange(0, ROT, 2, dtype=jnp.float32) / ROT)
    angles = jnp.arange(SEQ, dtype=jnp.float32)[:, None] * inv_freq[None, :]
    return jnp.cos(angles), jnp.sin(angles)


def rotary(head_vals, cos_t, sin_t):
    half_rot = ROT // 2
    first_half = head_vals[..., :half_rot]
    second_half = head_vals[..., half_rot:ROT]
    cos_b = cos_t[None, :, None, :]
    sin_b = sin_t[None, :, None, :]
    return jnp.concatenate([first_half * cos_b - second_half * sin_b, second_half * cos_b + first_half * sin_b, head_vals[..., ROT:]], axis=-1)


def causal_attention(q_all, k_all, v_all):
    n_blocks = SEQ // QBLK
    key_pos = jnp.arange(SEQ)

    def one_block(flat_idx):
        b_idx = flat_idx // n_blocks
        q_start = (flat_idx % n_blocks) * QBLK
        q_blk = lax.dynamic_slice(q_all, (b_idx, q_start, 0, 0), (1, QBLK, HEADS, HEAD))[0]
        k_row = lax.dynamic_index_in_dim(k_all, b_idx, axis=0, keepdims=False)
        v_row = lax.dynamic_index_in_dim(v_all, b_idx, axis=0, keepdims=False)
        scores = jnp.einsum('qhe,khe->hqk', q_blk, k_row) * HEAD ** -0.5
        q_pos = q_start + jnp.arange(QBLK)
        scores = jnp.where(key_pos[None, None, :] <= q_pos[None, :, None], scores, NEG_BIG)
        attn_probs = jax.nn.softmax(scores, axis=-1)
        return jnp.einsum('hqk,khe->qhe', attn_probs, v_row)

    block_outs = lax.map(jax.checkpoint(one_block), jnp.arange(BATCH * n_blocks))
    return block_outs.reshape(BATCH, SEQ, HEADS, HEAD)


def layer_forward(x_rows, ln1_gain, ln1_bias, ln2_gain, ln2_bias, w_qkv, b_qkv, w_out, b_out, w_up, b_up, w_down, b_down):
    cos_t, sin_t = rope_tables()
    h_attn = as_stored(layer_norm(x_rows, ln1_gain, ln1_bias))
    qkv_rows = jnp.einsum('bsd,dhce->bshce', h_attn, w_qkv) + b_qkv
    q_all = as_stored(rotary(qkv_rows[:, :, :, 0], cos_t, sin_t))
    k_all = as_stored(rotary(qkv_rows[:, :, :, 1], cos_t, sin_t))
    v_all = as_stored(qkv_rows[:, :, :, 2])
    attn_ctx = as_stored(causal_attention(q_all, k_all, v_all)).reshape(BATCH, SEQ, D)
    attn_proj = jnp.dot(attn_ctx, w_out) + b_out
    h_mlp = as_stored(layer_norm(x_rows, ln2_gain, ln2_bias))
    gelu_out = as_stored(jax.nn.gelu(jnp.dot(h_mlp, w_up) + b_up, approximate=False))
    mlp_proj = jnp.dot(gelu_out, w_down) + b_down
    return x_rows + attn_proj + mlp_proj


def reference(x_seq, dy_seq, ln1_gain, ln1_bias, ln2_gain, ln2_bias, w_qkv, b_qkv, w_out, b_out, w_up, b_up, w_down, b_down):
    y_full, back_fn = jax.vjp(layer_forward, x_seq.astype(jnp.float32), ln1_gain, ln1_bias, ln2_gain, ln2_bias, w_qkv.astype(jnp.float32), b_qkv.astype(jnp.float32), w_out.astype(jnp.float32), b_out.astype(jnp.float32), w_up.astype(jnp.float32), b_up.astype(jnp.float32), w_down.astype(jnp.float32), b_down.astype(jnp.float32))
    grads = back_fn(dy_seq)
    return (y_full.astype(jnp.bfloat16), grads[0], grads[1], grads[2], grads[3], grads[4], grads[5], grads[6], grads[7], grads[8], grads[9], grads[10], grads[11], grads[12])
```

```python
import functools

import jax
import jax.numpy as jnp
from jax import lax
from jax.experimental import pallas as pl
from jax.experimental.pallas import tpu as pltpu
from jax.sharding import PartitionSpec as P

EPS = 1e-5
ROPE_BASE = 10000.0
NEG_BIG = -1e30
VMEM_LIMIT = 60 * 1024 * 1024
NN = (((1,), (0,)), ((), ()))
NT = (((1,), (1,)), ((), ()))


def mm(a, b, dims=NN):
    return lax.dot_general(a, b, dims, preferred_element_type=jnp.float32)


def layer_norm(row_vals, norm_gain, norm_shift):
    row_mean = jnp.mean(row_vals, axis=-1, keepdims=True)
    centered = row_vals - row_mean
    inv_std = lax.rsqrt(jnp.mean(centered * centered, axis=-1, keepdims=True) + EPS)
    x_norm = centered * inv_std
    return x_norm * norm_gain + norm_shift, x_norm, inv_std


def norm_backward(d_out, x_norm, inv_std, norm_gain):
    d_norm = d_out * norm_gain
    d_rows = inv_std * (d_norm - jnp.mean(d_norm, axis=-1, keepdims=True) - x_norm * jnp.mean(d_norm * x_norm, axis=-1, keepdims=True))
    return d_rows, jnp.sum(d_out * x_norm, axis=0), jnp.sum(d_out, axis=0)


def rope_angles(positions, head_dim):
    rot_dim = head_dim // 4
    inv_freq = ROPE_BASE ** (-2.0 * jnp.arange(rot_dim // 2, dtype=jnp.float32) / rot_dim)
    return positions.astype(jnp.float32)[:, None] * inv_freq[None, :]


def lane_tables(cos_t, sin_t, head_dim):
    rows, half = cos_t.shape
    rest = head_dim - 2 * half
    one = jnp.concatenate([cos_t, cos_t, jnp.ones((rows, rest), jnp.float32)], axis=1)
    two = jnp.concatenate([-sin_t, sin_t, jnp.zeros((rows, rest), jnp.float32)], axis=1)
    return jnp.concatenate([one, one], axis=1), jnp.concatenate([two, two], axis=1)


def rotate(z, cos_l, sin_l, half, head_dim):
    lane = lax.broadcasted_iota(jnp.int32, cos_l.shape, 1) % head_dim
    low = lane < half
    parts = []
    for t in range(z.shape[1] // 128):
        zt = z[:, t * 128:(t + 1) * 128]
        partner = jnp.where(low, pltpu.roll(zt, 128 - half, 1), pltpu.roll(zt, half, 1))
        parts.append(zt * cos_l + partner * sin_l)
    return jnp.concatenate(parts, axis=1)


def exact_gelu(pre):
    cdf = 0.5 * (1.0 + lax.erf(pre * (0.5 ** 0.5)))
    pdf = jnp.exp(-0.5 * pre * pre) * 0.3989422804014327
    return pre * cdf, cdf + pre * pdf


def put_masked(dst, mat_t, hd):
    pairs = mat_t.shape[0] // (2 * hd)
    rows = lax.broadcasted_iota(jnp.int32, (2 * hd, mat_t.shape[1]), 0)
    for p in range(pairs):
        blk = mat_t[p * 2 * hd:(p + 1) * 2 * hd]
        zero = jnp.zeros_like(blk)
        dst[2 * p] = jnp.where(rows < hd, blk, zero)
        dst[2 * p + 1] = jnp.where(rows < hd, zero, blk)


def fwd_kernel(hd, me_ref, x_hbm, cos_hbm, sin_hbm, g_ref, s_ref, wq_ref, wk_ref, wv_ref, b_ref,
               k_hbm, v_hbm, ctx_ref, lse_ref, qt_ref,
               xb, cb, sb, kst, vst, qtm, acc, mrow, lrow, in_sem, out_sem):
    me = me_ref[0]
    T = xb.shape[1]
    W = xb.shape[2]
    heads = W // hd
    half = hd // 8
    scale = hd ** -0.5

    def fetch(j, slot):
        return (pltpu.make_async_copy(x_hbm.at[pl.ds(j * T, T)], xb.at[slot], in_sem.at[slot, 0]),
                pltpu.make_async_copy(cos_hbm.at[pl.ds(j * T, T)], cb.at[slot], in_sem.at[slot, 1]),
                pltpu.make_async_copy(sin_hbm.at[pl.ds(j * T, T)], sb.at[slot], in_sem.at[slot, 2]))

    def flush(j, slot):
        return (pltpu.make_async_copy(kst.at[slot], k_hbm.at[pl.ds(j * T, T)], out_sem.at[slot, 0]),
                pltpu.make_async_copy(vst.at[slot], v_hbm.at[pl.ds(j * T, T)], out_sem.at[slot, 1]))

    def project(slot, with_q):
        h = layer_norm(xb[slot].astype(jnp.float32), g_ref[...], s_ref[...])[0].astype(jnp.bfloat16)
        k = rotate(mm(h, wk_ref[...]) + b_ref[1:2], cb[slot], sb[slot], half, hd)
        kst[slot] = k.astype(jnp.bfloat16)
        vst[slot] = (mm(h, wv_ref[...]) + b_ref[2:3]).astype(jnp.bfloat16)
        if with_q:
            q = rotate(mm(h, wq_ref[...]) + b_ref[0:1], cb[slot], sb[slot], half, hd)
            q = q.astype(jnp.bfloat16) * jnp.bfloat16(scale)
            qt = q.T
            qt_ref[...] = qt
            put_masked(qtm, qt, hd)

    def attend(slot, diag):
        if diag:
            keep = lax.broadcasted_iota(jnp.int32, (T, T), 0) <= lax.broadcasted_iota(jnp.int32, (T, T), 1)
        for p in range(heads // 2):
            cols = slice(p * 2 * hd, (p + 1) * 2 * hd)
            kp = kst[slot, :, cols]
            vt = vst[slot, :, cols].T
            for h in (2 * p, 2 * p + 1):
                s = mm(kp, qtm[h])
                rows = slice(h * hd, (h + 1) * hd)
                vh = vt[(h % 2) * hd:(h % 2 + 1) * hd]
                if diag:
                    s = jnp.where(keep, s, NEG_BIG)
                    m = jnp.max(s, axis=0, keepdims=True)
                    e = jnp.exp(s - m)
                    lrow[h:h + 1] = jnp.sum(e, axis=0, keepdims=True)
                    acc[rows] = mm(vh, e.astype(jnp.bfloat16))
                else:
                    m_old = mrow[h:h + 1]
                    m = jnp.maximum(m_old, jnp.max(s, axis=0, keepdims=True))
                    e = jnp.exp(s - m)
                    alpha = jnp.exp(m_old - m)
                    lrow[h:h + 1] = lrow[h:h + 1] * alpha + jnp.sum(e, axis=0, keepdims=True)
                    acc[rows] = acc[rows] * alpha + mm(vh, e.astype(jnp.bfloat16))
                mrow[h:h + 1] = m

    for c in fetch(me, 0):
        c.start()

    @pl.when(me > 0)
    def _():
        for c in fetch(0, 1):
            c.start()

    for c in fetch(me, 0):
        c.wait()
    project(0, True)
    for c in flush(me, 0):
        c.start()
    attend(0, True)
    for c in flush(me, 0):
        c.wait()

    def step(j, _):
        slot = (j + 1) % 2

        @pl.when(j + 1 < me)
        def _():
            for c in fetch(j + 1, 1 - slot):
                c.start()

        for c in fetch(j, slot):
            c.wait()

        @pl.when(j >= 2)
        def _():
            for c in flush(j - 2, slot):
                c.wait()

        project(slot, False)
        for c in flush(j, slot):
            c.start()
        attend(slot, False)
        return 0

    lax.fori_loop(0, me, step, 0)

    @pl.when(me >= 1)
    def _():
        for c in flush(me - 1, me % 2):
            c.wait()

    @pl.when(me >= 2)
    def _():
        for c in flush(me - 2, (me + 1) % 2):
            c.wait()

    lse_ref[...] = mrow[...] + jnp.log(lrow[...])
    inv = 1.0 / lrow[...]
    for p in range(heads // 2):
        a = acc[2 * p * hd:(2 * p + 1) * hd] * inv[2 * p:2 * p + 1]
        b = acc[(2 * p + 1) * hd:(2 * p + 2) * hd] * inv[2 * p + 1:2 * p + 2]
        ctx_ref[:, 2 * p * hd:(2 * p + 2) * hd] = jnp.concatenate([a, b], axis=0).T


def fwd_attention(me, x_all, cos_l, sin_l, gain, shift, wq, wk, wv, b3, T, hd):
    S, W = x_all.shape
    heads = W // hd
    vm = pl.BlockSpec(memory_space=pltpu.VMEM)
    anym = pl.BlockSpec(memory_space=pl.ANY)
    f32, bf = jnp.float32, jnp.bfloat16
    return pl.pallas_call(
        functools.partial(fwd_kernel, hd),
        out_shape=[jax.ShapeDtypeStruct((S, W), bf), jax.ShapeDtypeStruct((S, W), bf), jax.ShapeDtypeStruct((T, W), f32),
                   jax.ShapeDtypeStruct((heads, T), f32), jax.ShapeDtypeStruct((W, T), bf)],
        in_specs=[pl.BlockSpec(memory_space=pltpu.SMEM), anym, anym, anym] + [vm] * 6,
        out_specs=[anym, anym, vm, vm, vm],
        scratch_shapes=[pltpu.VMEM((2, T, W), bf), pltpu.VMEM((2, T, 128), f32), pltpu.VMEM((2, T, 128), f32),
                        pltpu.VMEM((2, T, W), bf), pltpu.VMEM((2, T, W), bf), pltpu.VMEM((heads, 2 * hd, T), bf),
                        pltpu.VMEM((W, T), f32), pltpu.VMEM((heads, T), f32), pltpu.VMEM((heads, T), f32),
                        pltpu.SemaphoreType.DMA((2, 3)), pltpu.SemaphoreType.DMA((2, 2))],
        compiler_params=pltpu.CompilerParams(vmem_limit_bytes=VMEM_LIMIT),
        cost_estimate=pl.CostEstimate(flops=40_000_000_000, bytes_accessed=40_000_000, transcendentals=0),
        name="attn_fwd",
    )(me, x_all, cos_l, sin_l, gain, shift, wq, wk, wv, b3)


def bwd_kernel(hd, n, me_ref, x_hbm, dy_hbm, cos_hbm, sin_hbm, k_hbm, v_hbm, stats_ref, qt_ref, own_ref, g_ref, s_ref,
               wq_ref, wot_ref, bq_ref, dq_ref, dk_ref, dv_ref,
               xb, yb, cb, sb, qsc, osc, am, bm, acc1, acc2, in_sem):
    me = me_ref[0]
    T = xb.shape[1]
    W = xb.shape[2]
    heads = W // hd
    half = hd // 8
    scale = hd ** -0.5

    def fetch_kv(j, slot):
        return (pltpu.make_async_copy(k_hbm.at[pl.ds(j * T, T)], xb.at[slot], in_sem.at[slot, 0]),
                pltpu.make_async_copy(v_hbm.at[pl.ds(j * T, T)], yb.at[slot], in_sem.at[slot, 1]))

    def fetch_xy(j, slot):
        return (pltpu.make_async_copy(x_hbm.at[pl.ds(j * T, T)], xb.at[slot], in_sem.at[slot, 0]),
                pltpu.make_async_copy(dy_hbm.at[pl.ds(j * T, T)], yb.at[slot], in_sem.at[slot, 1]),
                pltpu.make_async_copy(cos_hbm.at[pl.ds(j * T, T)], cb.at[slot], in_sem.at[slot, 2]),
                pltpu.make_async_copy(sin_hbm.at[pl.ds(j * T, T)], sb.at[slot], in_sem.at[slot, 3]))

    low_tri = lambda: lax.broadcasted_iota(jnp.int32, (T, T), 0) <= lax.broadcasted_iota(jnp.int32, (T, T), 1)

    put_masked(am, qt_ref[...], hd)
    put_masked(bm, own_ref[...].T, hd)
    acc1[...] = jnp.zeros_like(acc1)

    def dq_block(slot, diag):
        for p in range(heads // 2):
            cols = slice(p * 2 * hd, (p + 1) * 2 * hd)
            kp = xb[slot, :, cols]
            vp = yb[slot, :, cols]
            kt = kp.T
            for h in (2 * p, 2 * p + 1):
                row = pl.ds(me * 2 * heads + h, 1)
                s = mm(kp, am[h])
                if diag:
                    s = jnp.where(low_tri(), s, NEG_BIG)
                pr = jnp.exp(s - stats_ref[row, :])
                dp = mm(vp, bm[h])
                ds = (pr * (dp - stats_ref[pl.ds(me * 2 * heads + heads + h, 1), :])).astype(jnp.bfloat16)
                acc1[h * hd:(h + 1) * hd] += mm(kt[(h % 2) * hd:(h % 2 + 1) * hd], ds)

    for c in fetch_kv(0, 0):
        c.start()

    def dq_step(j, _):
        slot = j % 2
        for c in fetch_kv(j + 1, 1 - slot):
            c.start()
        for c in fetch_kv(j, slot):
            c.wait()
        dq_block(slot, False)
        return 0

    lax.fori_loop(0, me, dq_step, 0)
    last = me % 2
    for c in fetch_kv(me, last):
        c.wait()
    for c in fetch_xy(me, 1 - last):
        c.start()
    dq_block(last, True)
    dq_ref[...] = acc1[...].T * scale

    put_masked(am, xb[last].T, hd)
    put_masked(bm, yb[last].T, hd)
    acc1[...] = jnp.zeros_like(acc1)
    acc2[...] = jnp.zeros_like(acc2)

    def dkv_block(j, slot, diag):
        h_rows = layer_norm(xb[slot].astype(jnp.float32), g_ref[...], s_ref[...])[0].astype(jnp.bfloat16)
        q = rotate(mm(h_rows, wq_ref[...]) + bq_ref[...], cb[slot], sb[slot], half, hd)
        qsc[...] = q.astype(jnp.bfloat16) * jnp.bfloat16(scale)
        osc[...] = mm(yb[slot], wot_ref[...]).astype(jnp.bfloat16)
        st = stats_ref[pl.ds(j * 2 * heads, 2 * heads), :].T
        for p in range(heads // 2):
            cols = slice(p * 2 * hd, (p + 1) * 2 * hd)
            qp = qsc[:, cols]
            op = osc[:, cols]
            qt = qp.T
            ot = op.T
            for h in (2 * p, 2 * p + 1):
                s = mm(qp, am[h])
                if diag:
                    s = jnp.where(jnp.logical_not(low_tri()) | (lax.broadcasted_iota(jnp.int32, (T, T), 0) == lax.broadcasted_iota(jnp.int32, (T, T), 1)), s, NEG_BIG)
                pr = jnp.exp(s - st[:, h:h + 1])
                half_rows = slice((h % 2) * hd, (h % 2 + 1) * hd)
                rows = slice(h * hd, (h + 1) * hd)
                acc2[rows] += mm(ot[half_rows], pr.astype(jnp.bfloat16))
                dp = mm(op, bm[h])
                ds = (pr * (dp - st[:, heads + h:heads + h + 1])).astype(jnp.bfloat16)
                acc1[rows] += mm(qt[half_rows], ds)

    first = 1 - last

    @pl.when(me + 1 < n)
    def _():
        for c in fetch_xy(me + 1, 1 - first):
            c.start()

    for c in fetch_xy(me, first):
        c.wait()
    dkv_block(me, first, True)

    def dkv_step(j, _):
        slot = (j - me + first) % 2

        @pl.when(j + 1 < n)
        def _():
            for c in fetch_xy(j + 1, 1 - slot):
                c.start()

        for c in fetch_xy(j, slot):
            c.wait()
        dkv_block(j, slot, False)
        return 0

    lax.fori_loop(me + 1, n, dkv_step, 0)
    dk_ref[...] = acc1[...].T
    dv_ref[...] = acc2[...].T


def bwd_attention(me, x_all, dy_all, cos_l, sin_l, k_all, v_all, stats, qt, d_ctx_bf, gain, shift, wq, wot, bq, T, hd):
    S, W = x_all.shape
    heads = W // hd
    vm = pl.BlockSpec(memory_space=pltpu.VMEM)
    anym = pl.BlockSpec(memory_space=pl.ANY)
    f32, bf = jnp.float32, jnp.bfloat16
    return pl.pallas_call(
        functools.partial(bwd_kernel, hd, S // T),
        out_shape=[jax.ShapeDtypeStruct((T, W), f32)] * 3,
        in_specs=[pl.BlockSpec(memory_space=pltpu.SMEM)] + [anym] * 6 + [vm] * 8,
        out_specs=[vm] * 3,
        scratch_shapes=[pltpu.VMEM((2, T, W), bf), pltpu.VMEM((2, T, W), bf), pltpu.VMEM((2, T, 128), f32), pltpu.VMEM((2, T, 128), f32),
                        pltpu.VMEM((T, W), bf), pltpu.VMEM((T, W), bf), pltpu.VMEM((heads, 2 * hd, T), bf), pltpu.VMEM((heads, 2 * hd, T), bf),
                        pltpu.VMEM((W, T), f32), pltpu.VMEM((W, T), f32), pltpu.SemaphoreType.DMA((2, 4))],
        compiler_params=pltpu.CompilerParams(vmem_limit_bytes=VMEM_LIMIT),
        cost_estimate=pl.CostEstimate(flops=80_000_000_000, bytes_accessed=40_000_000, transcendentals=0),
        name="attn_bwd",
    )(me, x_all, dy_all, cos_l, sin_l, k_all, v_all, stats, qt, d_ctx_bf, gain, shift, wq, wot, bq)


def mlp_kernel(x_ref, dy_ref, g_ref, s_ref, wu_ref, bu_ref, wd_ref, du_ref, dd_ref, db_ref):
    @pl.when(pl.program_id(0) == 0)
    def _():
        du_ref[...] = jnp.zeros_like(du_ref)
        dd_ref[...] = jnp.zeros_like(dd_ref)
        db_ref[...] = jnp.zeros_like(db_ref)

    h = layer_norm(x_ref[...].astype(jnp.float32), g_ref[...], s_ref[...])[0].astype(jnp.bfloat16)
    dy = dy_ref[...]
    act, slope = exact_gelu(mm(h, wu_ref[...]) + bu_ref[...])
    d_up = mm(dy, wd_ref[...]) * slope
    keep = du_ref.shape[0]
    db_ref[...] += jnp.sum(d_up, axis=0, keepdims=True)
    du_ref[...] += mm(d_up.astype(jnp.bfloat16).T, h)[:keep]
    dd_ref[...] += mm(act.astype(jnp.bfloat16).T, dy)[:keep]


def mlp_grads(x_all, dy_all, gain, shift, wu, bu, wd, keep):
    S, W = x_all.shape
    F = wu.shape[1]
    R = 512
    const = lambda j: (0, 0)
    return pl.pallas_call(
        mlp_kernel,
        grid=(S // R,),
        out_shape=[jax.ShapeDtypeStruct((keep, W), jnp.float32)] * 2 + [jax.ShapeDtypeStruct((1, F), jnp.float32)],
        in_specs=[pl.BlockSpec((R, W), lambda j: (j, 0)), pl.BlockSpec((R, W), lambda j: (j, 0)), pl.BlockSpec((1, W), const), pl.BlockSpec((1, W), const),
                  pl.BlockSpec((W, F), const), pl.BlockSpec((1, F), const), pl.BlockSpec((W, F), const)],
        out_specs=[pl.BlockSpec((keep, W), const)] * 2 + [pl.BlockSpec((1, F), const)],
        compiler_params=pltpu.CompilerParams(vmem_limit_bytes=VMEM_LIMIT, dimension_semantics=("arbitrary",)),
        cost_estimate=pl.CostEstimate(flops=20_000_000_000, bytes_accessed=26_000_000, transcendentals=0),
        name="mlp_grads",
    )(x_all, dy_all, gain, shift, wu, bu, wd)


def solution(mesh):
    cp_size = mesh.shape['cp']
    row_spec = P('dp', 'cp', None)
    in_specs = (row_spec, row_spec) + (P(),) * 12
    out_specs = (row_spec, row_spec, P('dp'), P('dp'), P('dp'), P('dp'), P('dp', None, None, None), P('dp', None, None), P('dp', None), P('dp'), P('dp', None), P('dp'), P('dp', None), P('dp'))
    bf, f32 = jnp.bfloat16, jnp.float32

    def local_layer(x_blk, dy_blk, ln1_gain, ln1_bias, ln2_gain, ln2_bias, w_qkv, b_qkv, w_out, b_out, w_up, b_up, w_down, b_down):
        T, W = x_blk.shape[1:]
        heads, hd = w_qkv.shape[1], w_qkv.shape[3]
        FF = w_up.shape[1]
        S = T * cp_size
        me = lax.axis_index('cp')
        me1 = me.astype(jnp.int32).reshape(1)
        row = lambda v: v.reshape(1, -1).astype(f32)

        x_own = x_blk[0]
        dy_own = dy_blk[0]
        dy_bf = dy_own.astype(bf)
        x_all = lax.all_gather(x_own, 'cp', tiled=True)
        dy_all = lax.all_gather(dy_bf, 'cp', tiled=True)

        w3 = w_qkv.transpose(2, 0, 1, 3).reshape(3, W, W)
        b3 = b_qkv.astype(f32).transpose(1, 0, 2).reshape(3, W)
        ang = rope_angles(jnp.arange(S), hd)
        cos_l, sin_l = lane_tables(jnp.cos(ang), jnp.sin(ang), hd)

        x_rows = x_own.astype(f32)
        h_attn, x_norm1, inv_std1 = layer_norm(x_rows, ln1_gain, ln1_bias)
        h_attn = h_attn.astype(bf)
        h_mlp, x_norm2, inv_std2 = layer_norm(x_rows, ln2_gain, ln2_bias)
        h_mlp = h_mlp.astype(bf)
        gelu_out, slope = exact_gelu(mm(h_mlp, w_up) + b_up.astype(f32))
        mlp_proj = mm(gelu_out.astype(bf), w_down) + b_down.astype(f32)
        d_up_bf = (mm(dy_bf, w_down, NT) * slope).astype(bf)
        d_h_mlp = mm(d_up_bf, w_up, NT)
        d_ctx = mm(dy_bf, w_out, NT)
        dx_mlp, d_ln2_gain, d_ln2_bias = norm_backward(d_h_mlp, x_norm2, inv_std2, ln2_gain)

        k_all, v_all, attn_norm, lse, qt = fwd_attention(me1, x_all, cos_l, sin_l, row(ln1_gain), row(ln1_bias), w3[0], w3[1], w3[2], b3, T, hd)
        delta = jnp.sum((d_ctx * attn_norm).reshape(T, heads, hd), axis=-1).T
        stats = lax.all_gather(jnp.concatenate([lse, delta], axis=0), 'cp', tiled=True)
        attn_ctx = attn_norm.astype(bf)
        y_rows = (x_rows + (mm(attn_ctx, w_out) + b_out.astype(f32)) + mlp_proj).astype(bf)
        d_w_out = mm(attn_ctx, dy_bf, (((0,), (0,)), ((), ())))

        F = FF // cp_size
        F_pad = -(-F // 128) * 128
        pad = lambda a, ax: jnp.pad(a, [(0, F_pad - F) if d == ax else (0, 0) for d in range(a.ndim)])
        wu_s = pad(lax.dynamic_slice_in_dim(w_up, me * F, F, 1), 1)
        bu_s = pad(lax.dynamic_slice_in_dim(b_up.astype(f32), me * F, F, 0), 0).reshape(1, F_pad)
        wd_s = pad(lax.dynamic_slice_in_dim(w_down, me * F, F, 0).T, 1)
        du_s, dd_s, db_s = mlp_grads(x_all, dy_all, row(ln2_gain), row(ln2_bias), wu_s, bu_s, wd_s, F)
        d_w_up = lax.all_gather(du_s, 'cp', tiled=True).T
        d_w_down = lax.all_gather(dd_s, 'cp', tiled=True)
        d_b_up = lax.dynamic_update_slice(jnp.zeros((FF,), f32), db_s[0, :F], (me * F,))

        d_q, d_k, d_v = bwd_attention(me1, x_all, dy_all, cos_l, sin_l, k_all, v_all, stats, qt, d_ctx.astype(bf), row(ln1_gain), row(ln1_bias), w3[0], w_out.T, b3[0:1], T, hd)
        cos_o = lax.dynamic_slice_in_dim(cos_l, me * T, T, 0)[:, None, :hd]
        sin_o = lax.dynamic_slice_in_dim(sin_l, me * T, T, 0)[:, None, :hd]
        half = hd // 8

        def unrotate(g):
            g = g.reshape(T, heads, hd)
            partner = jnp.concatenate([g[..., half:2 * half], g[..., :half], g[..., 2 * half:]], axis=-1)
            return (g * cos_o - partner * sin_o).reshape(T, W)

        d3 = jnp.concatenate([unrotate(d_q), unrotate(d_k), d_v], axis=1)
        d_b_qkv = jnp.sum(d3, axis=0).reshape(3, heads, hd).transpose(1, 0, 2)
        d3_bf = d3.astype(bf)
        d_w3 = mm(h_attn, d3_bf, (((0,), (0,)), ((), ())))
        d_h_attn = mm(d3_bf, w3.transpose(0, 2, 1).reshape(3 * W, W))
        dx_attn, d_ln1_gain, d_ln1_bias = norm_backward(d_h_attn, x_norm1, inv_std1, ln1_gain)
        dx_rows = dy_own + dx_attn + dx_mlp

        d_w_qkv = d_w3.reshape(W, 3, heads, hd).transpose(0, 2, 1, 3)
        dy_sum = jnp.sum(dy_own, axis=0)
        summed = lax.psum((d_ln1_gain, d_ln1_bias, d_ln2_gain, d_ln2_bias, d_w_qkv, d_b_qkv, d_w_out, dy_sum, d_b_up), 'cp')
        return (y_rows[None], dx_rows[None]) + tuple(summed[:8]) + (d_w_up, summed[8], d_w_down, summed[7])

    return jax.shard_map(local_layer, mesh=mesh, in_specs=in_specs, out_specs=out_specs, check_vma=False)
```

```python
import functools

import jax
import jax.numpy as jnp
from jax import lax
from jax.experimental import pallas as pl
from jax.experimental.pallas import tpu as pltpu
from jax.sharding import PartitionSpec as P

EPS = 1e-5
ROPE_BASE = 10000.0
NEG_BIG = -1e30
VMEM_LIMIT = 60 * 1024 * 1024
NN = (((1,), (0,)), ((), ()))
NT = (((1,), (1,)), ((), ()))


def mm(a, b, dims=NN):
    return lax.dot_general(a, b, dims, preferred_element_type=jnp.float32)


def layer_norm(row_vals, norm_gain, norm_shift):
    row_mean = jnp.mean(row_vals, axis=-1, keepdims=True)
    centered = row_vals - row_mean
    inv_std = lax.rsqrt(jnp.mean(centered * centered, axis=-1, keepdims=True) + EPS)
    x_norm = centered * inv_std
    return x_norm * norm_gain + norm_shift, x_norm, inv_std


def norm_backward(d_out, x_norm, inv_std, norm_gain):
    d_norm = d_out * norm_gain
    d_rows = inv_std * (d_norm - jnp.mean(d_norm, axis=-1, keepdims=True) - x_norm * jnp.mean(d_norm * x_norm, axis=-1, keepdims=True))
    return d_rows, jnp.sum(d_out * x_norm, axis=0), jnp.sum(d_out, axis=0)


def rope_angles(positions, head_dim):
    rot_dim = head_dim // 4
    inv_freq = ROPE_BASE ** (-2.0 * jnp.arange(rot_dim // 2, dtype=jnp.float32) / rot_dim)
    return positions.astype(jnp.float32)[:, None] * inv_freq[None, :]


def lane_tables(positions, head_dim):
    rot_dim = head_dim // 4
    freq = ROPE_BASE ** (-2.0 * jnp.arange(rot_dim // 2, dtype=jnp.float32) / rot_dim)
    rest = jnp.zeros((head_dim // 2 - rot_dim // 2,), jnp.float32)
    lanes = jnp.concatenate([-freq, rest, -freq, rest, freq, rest, freq, rest])
    angles = positions.astype(jnp.float32)[:, None] * lanes[None, :]
    return jnp.cos(angles), jnp.sin(angles)


def turn(tab, j, cs, ss):
    cl, sl, cb, sb = tab
    ca, sa = cb[pl.ds(j, 1), :], sb[pl.ds(j, 1), :]
    cs[...] = ca * cl[...] - sa * sl[...]
    ss[...] = sa * cl[...] + ca * sl[...]


def pair_rows(w_t):
    heads, hd = w_t.shape[:2]
    half = hd // 8
    mid = (hd - 2 * half) // 2 + 2 * half
    low = jnp.concatenate([w_t[:, :half], w_t[:, 2 * half:mid]], axis=1)
    high = jnp.concatenate([w_t[:, half:2 * half], w_t[:, mid:]], axis=1)
    both = jnp.stack([low, high], axis=1).reshape(heads // 2, 2, 2, hd // 2, -1)
    return both.transpose(0, 2, 1, 3, 4).reshape(heads * hd, -1)


def rotate(z, cos_l, sin_l):
    parts = []
    for t in range(z.shape[1] // 128):
        zt = z[:, t * 128:(t + 1) * 128]
        parts.append(zt * cos_l + pltpu.roll(zt, 64, 1) * sin_l)
    return jnp.concatenate(parts, axis=1)


def exact_gelu(pre):
    cdf = 0.5 * (1.0 + lax.erf(pre * (0.5 ** 0.5)))
    pdf = jnp.exp(-0.5 * pre * pre) * 0.3989422804014327
    return pre * cdf, cdf + pre * pdf


def put_masked(dst, mat_t, hd, paired):
    rows = lax.broadcasted_iota(jnp.int32, (2 * hd, mat_t.shape[1]), 0)
    first = (rows % hd < hd // 2) if paired else (rows < hd)
    for p in range(mat_t.shape[0] // (2 * hd)):
        blk = mat_t[p * 2 * hd:(p + 1) * 2 * hd]
        zero = jnp.zeros_like(blk)
        dst[2 * p] = jnp.where(first, blk, zero)
        dst[2 * p + 1] = jnp.where(first, zero, blk)


def head_rows(mat_t, i, hd, paired):
    if not paired:
        return mat_t[i * hd:(i + 1) * hd]
    q = hd // 2
    return jnp.concatenate([mat_t[i * q:(i + 1) * q], mat_t[hd + i * q:hd + (i + 1) * q]], axis=0)


def causal(T, keys_first):
    r = lax.broadcasted_iota(jnp.int32, (T, T), 0)
    c = lax.broadcasted_iota(jnp.int32, (T, T), 1)
    return (r <= c) if keys_first else (c <= r)


def fwd_kernel(hd, me_ref, x_hbm, cl_ref, sl_ref, cb_ref, sb_ref, g_ref, s_ref, wq_ref, wk_ref, wv_ref, b_ref,
               k_hbm, v_hbm, ctx_ref, lse_ref, qt_ref,
               xb, cs, ss, hsc, kst, vst, qtm, sbuf, acc, mrow, lrow, in_sem, out_sem):
    me = me_ref[0]
    T = xb.shape[1]
    W = xb.shape[2]
    pairs = W // (2 * hd)
    scale = hd ** -0.5
    tiles = W // 256

    tab = (cl_ref, sl_ref, cb_ref, sb_ref)
    DEEP = xb.shape[0]

    def fetch(j):
        blk = jnp.where(j < 0, me, jnp.minimum(j, me))
        slot = (j + 1) % DEEP
        return (pltpu.make_async_copy(x_hbm.at[pl.ds(blk * T, T)], xb.at[slot], in_sem.at[slot]),)

    def flush(j, slot):
        return (pltpu.make_async_copy(kst.at[slot], k_hbm.at[pl.ds(j * T, T)], out_sem.at[slot, 0]),
                pltpu.make_async_copy(vst.at[slot], v_hbm.at[pl.ds(j * T, T)], out_sem.at[slot, 1]))

    def start(copies):
        for c in copies:
            c.start()

    def wait(copies):
        for c in copies:
            c.wait()

    def norm(j):
        hsc[...] = layer_norm(xb[(j + 1) % DEEP].astype(jnp.float32), g_ref[...], s_ref[...])[0].astype(jnp.bfloat16)
        turn(tab, jnp.where(j < 0, me, j), cs, ss)

    def piece(i, slot):
        cols = slice((i % tiles) * 256, (i % tiles + 1) * 256)
        if i < tiles:
            kst[slot, :, cols] = rotate(mm(hsc[...], wk_ref[:, cols]) + b_ref[1:2, cols], cs[...], ss[...]).astype(jnp.bfloat16)
        else:
            vst[slot, :, cols] = (mm(hsc[...], wv_ref[:, cols]) + b_ref[2:3, cols]).astype(jnp.bfloat16)

    def scores(slot, p):
        kp = kst[slot, :, p * 2 * hd:(p + 1) * 2 * hd]
        return [mm(kp, qtm[h]) for h in (2 * p, 2 * p + 1)]

    def attend(j, slot, diag):
        ahead = scores(slot, 0) if diag else [sbuf[0], sbuf[1]]
        norm(j + 1)
        per = -(-2 * tiles // pairs)
        for p in range(pairs):
            now = ahead
            for i in range(p * per, min((p + 1) * per, 2 * tiles)):
                piece(i, 1 - slot)
            if p + 1 < pairs:
                ahead = scores(slot, p + 1)
            else:
                ahead = scores(1 - slot, 0)
            vt = vst[slot, :, p * 2 * hd:(p + 1) * 2 * hd].T
            for i in range(2):
                h = 2 * p + i
                s = now[i]
                rows = slice(h * hd, (h + 1) * hd)
                vh = head_rows(vt, i, hd, False)
                if diag:
                    s = jnp.where(causal(T, True), s, NEG_BIG)
                    m = jnp.max(s, axis=0, keepdims=True)
                    e = jnp.exp(s - m)
                    lrow[h:h + 1] = jnp.sum(e, axis=0, keepdims=True)
                    acc[rows] = mm(vh, e.astype(jnp.bfloat16))
                else:
                    m_old = mrow[h:h + 1]
                    m = jnp.maximum(m_old, jnp.max(s, axis=0, keepdims=True))
                    e = jnp.exp(s - m)
                    alpha = jnp.exp(m_old - m)
                    lrow[h:h + 1] = lrow[h:h + 1] * alpha + jnp.sum(e, axis=0, keepdims=True)
                    acc[rows] = acc[rows] * alpha + mm(vh, e.astype(jnp.bfloat16))
                mrow[h:h + 1] = m
        sbuf[0] = ahead[0]
        sbuf[1] = ahead[1]

    for j in range(-1, DEEP - 1):
        start(fetch(jnp.int32(j)))
    own = jnp.int32(-1)
    wait(fetch(own))
    norm(own)
    for i in range(2 * tiles):
        piece(i, 0)
    for t in range(tiles):
        cols = slice(t * 256, (t + 1) * 256)
        q = rotate(mm(hsc[...], wq_ref[:, cols]) + b_ref[0:1, cols], cs[...], ss[...])
        qt_ref[cols] = (q.astype(jnp.bfloat16) * jnp.bfloat16(scale)).T
    put_masked(qtm, qt_ref[...], hd, True)
    start(flush(me, 0))
    start(fetch(own + DEEP))
    wait(fetch(own + 1))
    attend(own, 0, True)

    @pl.when(me >= 1)
    def _():
        start(flush(0, 1))

    wait(flush(me, 0))

    def step(j, slot):
        wait(fetch(j + 1))
        start(fetch(j + DEEP))

        @pl.when(j >= 1)
        def _():
            wait(flush(j - 1, 1 - slot))

        attend(j, slot, False)

        @pl.when(j + 1 < me)
        def _():
            start(flush(j + 1, 1 - slot))

        return 1 - slot

    last = lax.fori_loop(0, me, step, jnp.int32(1))

    for k in range(1, DEEP):
        wait(fetch(me + k))

    @pl.when(me >= 1)
    def _():
        wait(flush(me - 1, 1 - last))

    lse_ref[...] = mrow[...] + jnp.log(lrow[...])
    inv = 1.0 / lrow[...]
    for p in range(pairs):
        a = acc[2 * p * hd:(2 * p + 1) * hd] * inv[2 * p:2 * p + 1]
        b = acc[(2 * p + 1) * hd:(2 * p + 2) * hd] * inv[2 * p + 1:2 * p + 2]
        ctx_ref[:, 2 * p * hd:(2 * p + 2) * hd] = jnp.concatenate([a, b], axis=0).T


def fwd_attention(me, x_all, tab, gain, shift, wq, wk, wv, b3, T, hd):
    S, W = x_all.shape
    heads = W // hd
    vm = pl.BlockSpec(memory_space=pltpu.VMEM)
    anym = pl.BlockSpec(memory_space=pl.ANY)
    f32, bf = jnp.float32, jnp.bfloat16
    return pl.pallas_call(
        functools.partial(fwd_kernel, hd),
        out_shape=[jax.ShapeDtypeStruct((S, W), bf), jax.ShapeDtypeStruct((S, W), bf), jax.ShapeDtypeStruct((T, W), f32),
                   jax.ShapeDtypeStruct((heads, T), f32), jax.ShapeDtypeStruct((W, T), bf)],
        in_specs=[pl.BlockSpec(memory_space=pltpu.SMEM), anym] + [vm] * 10,
        out_specs=[anym, anym, vm, vm, vm],
        scratch_shapes=[pltpu.VMEM((4, T, W), bf), pltpu.VMEM((T, 128), f32), pltpu.VMEM((T, 128), f32), pltpu.VMEM((T, W), bf),
                        pltpu.VMEM((2, T, W), bf), pltpu.VMEM((2, T, W), bf), pltpu.VMEM((heads, 2 * hd, T), bf), pltpu.VMEM((2, T, T), f32),
                        pltpu.VMEM((W, T), f32), pltpu.VMEM((heads, T), f32), pltpu.VMEM((heads, T), f32),
                        pltpu.SemaphoreType.DMA((4,)), pltpu.SemaphoreType.DMA((2, 2))],
        compiler_params=pltpu.CompilerParams(vmem_limit_bytes=VMEM_LIMIT),
        cost_estimate=pl.CostEstimate(flops=40_000_000_000, bytes_accessed=40_000_000, transcendentals=0),
        name="attn_fwd",
    )(me, x_all, *tab, gain, shift, wq, wk, wv, b3)


def bwd_kernel(hd, n, heads, h0, width, srows, me_ref, x_hbm, dy_hbm, k_hbm, v_hbm, cl_ref, sl_ref, cb_ref, sb_ref, stats_ref, qt_ref, own_ref, g_ref, s_ref,
               wq_ref, wot_ref, bq_ref, ct_ref, st_ref, d3_ref,
               xb, yb, cs, ss, kb, vb, hsc, qsc, osc, am, bm, sbuf, acc1, acc2, kv_sem, xy_sem):
    me = me_ref[0]
    T = xb.shape[1]
    pairs = width // (2 * hd)
    half = hd // 8
    scale = hd ** -0.5
    c0 = h0 * hd

    tab = (cl_ref, sl_ref, cb_ref, sb_ref)
    DEEP = xb.shape[0]

    def fetch_kv(j):
        slot, blk = j % DEEP, jnp.minimum(j, me)
        return (pltpu.make_async_copy(k_hbm.at[pl.ds(blk * T, T), c0:c0 + width], kb.at[slot], kv_sem.at[slot, 0]),
                pltpu.make_async_copy(v_hbm.at[pl.ds(blk * T, T), c0:c0 + width], vb.at[slot], kv_sem.at[slot, 1]))

    def fetch_xy(r):
        slot, blk = r % DEEP, jnp.minimum(me + r, n - 1)
        return (pltpu.make_async_copy(x_hbm.at[pl.ds(blk * T, T)], xb.at[slot], xy_sem.at[slot, 0]),
                pltpu.make_async_copy(dy_hbm.at[pl.ds(blk * T, T)], yb.at[slot], xy_sem.at[slot, 1]))

    def start(copies):
        for c in copies:
            c.start()

    def wait(copies):
        for c in copies:
            c.wait()

    def pair_cols(p):
        return slice(p * 2 * hd, (p + 1) * 2 * hd)

    def unrotated(z):
        mid = hd // 2
        a, b = z[:half], z[mid:mid + half]
        ct, st = ct_ref[...], st_ref[...]
        return jnp.concatenate([a * ct + b * st, b * ct - a * st, z[half:mid], z[mid + half:]], axis=0)

    for r in range(DEEP - 1):
        start(fetch_kv(jnp.int32(r)))
    for r in range(DEEP):
        start(fetch_xy(jnp.int32(r)))
    put_masked(am, qt_ref[c0:c0 + width], hd, True)
    put_masked(bm, own_ref[:, c0:c0 + width].T, hd, False)
    acc1[...] = jnp.zeros_like(acc1)

    def dq_scores(slot, p):
        kp, vp = kb[slot, :, pair_cols(p)], vb[slot, :, pair_cols(p)]
        return [(mm(kp, am[h]), mm(vp, bm[h])) for h in (2 * p, 2 * p + 1)]

    def dq_block(slot, diag):
        ahead = dq_scores(slot, 0)
        for p in range(pairs):
            now = ahead
            if p + 1 < pairs:
                ahead = dq_scores(slot, p + 1)
            kt = kb[slot, :, pair_cols(p)].T
            for i in range(2):
                h = 2 * p + i
                s, dp = now[i]
                if diag:
                    s = jnp.where(causal(T, True), s, NEG_BIG)
                pr = jnp.exp(s - stats_ref[pl.ds(me * srows + h0 + h, 1), :])
                ds = (pr * (dp - stats_ref[pl.ds(me * srows + heads + h0 + h, 1), :])).astype(jnp.bfloat16)
                acc1[h * hd:(h + 1) * hd] += mm(head_rows(kt, i, hd, True), ds)

    def dq_step(j, _):
        start(fetch_kv(j + DEEP - 1))
        wait(fetch_kv(j))
        dq_block(j % DEEP, False)
        return 0

    lax.fori_loop(0, me, dq_step, 0)
    last = me % DEEP
    wait(fetch_kv(me))
    dq_block(last, True)
    for k in range(1, DEEP - 1):
        wait(fetch_kv(me + k))
    for h in range(2 * pairs):
        d3_ref[3 * h * hd:(3 * h + 1) * hd] = unrotated(acc1[h * hd:(h + 1) * hd] * scale)

    put_masked(am, kb[last].T, hd, True)
    put_masked(bm, vb[last].T, hd, False)
    acc1[...] = jnp.zeros_like(acc1)
    acc2[...] = jnp.zeros_like(acc2)

    tiles = width // 256

    def norm(r):
        hsc[...] = layer_norm(xb[r % DEEP].astype(jnp.float32), g_ref[...], s_ref[...])[0].astype(jnp.bfloat16)
        turn(tab, jnp.minimum(me + r, n - 1), cs, ss)

    def piece(i, r, slot):
        cols = slice(i // 2 * 256, (i // 2 + 1) * 256)
        if i % 2 == 0:
            q = rotate(mm(hsc[...], wq_ref[:, cols]) + bq_ref[:, cols], cs[...], ss[...])
            qsc[slot, :, cols] = q.astype(jnp.bfloat16) * jnp.bfloat16(scale)
        else:
            osc[slot, :, cols] = mm(yb[r % DEEP], wot_ref[:, cols]).astype(jnp.bfloat16)

    def dkv_scores(slot, p):
        qp, op = qsc[slot, :, pair_cols(p)], osc[slot, :, pair_cols(p)]
        return [(mm(qp, am[h]), mm(op, bm[h])) for h in (2 * p, 2 * p + 1)]

    def dkv_block(r, diag):
        j, slot = me + r, r % 2
        ahead = dkv_scores(slot, 0) if diag else [(sbuf[0], sbuf[1]), (sbuf[2], sbuf[3])]
        st = stats_ref[pl.ds(j * srows, srows), :].T
        norm(r + 1)
        per = -(-2 * tiles // pairs)
        for p in range(pairs):
            now = ahead
            for i in range(p * per, min((p + 1) * per, 2 * tiles)):
                piece(i, r + 1, 1 - slot)
            ahead = dkv_scores(slot, p + 1) if p + 1 < pairs else dkv_scores(1 - slot, 0)
            qt = qsc[slot, :, pair_cols(p)].T
            ot = osc[slot, :, pair_cols(p)].T
            for i in range(2):
                h = 2 * p + i
                s, dp = now[i]
                if diag:
                    s = jnp.where(causal(T, False), s, NEG_BIG)
                rows = slice(h * hd, (h + 1) * hd)
                pr = jnp.exp(s - st[:, h0 + h:h0 + h + 1])
                acc2[rows] += mm(head_rows(ot, i, hd, False), pr.astype(jnp.bfloat16))
                ds = (pr * (dp - st[:, heads + h0 + h:heads + h0 + h + 1])).astype(jnp.bfloat16)
                acc1[rows] += mm(head_rows(qt, i, hd, True), ds)
        for i in range(2):
            sbuf[2 * i] = ahead[i][0]
            sbuf[2 * i + 1] = ahead[i][1]

    zero = jnp.int32(0)
    wait(fetch_xy(zero))
    norm(zero)
    for i in range(2 * tiles):
        piece(i, zero, 0)

    def dkv_step(r, diag):
        wait(fetch_xy(r + 1))
        start(fetch_xy(r + DEEP))
        dkv_block(r, diag)
        return 0

    dkv_step(zero, True)
    lax.fori_loop(1, n - me, lambda r, _: dkv_step(r, False), 0)
    for k in range(1, DEEP):
        wait(fetch_xy(n - me + k))
    for h in range(2 * pairs):
        d3_ref[(3 * h + 1) * hd:(3 * h + 2) * hd] = unrotated(acc1[h * hd:(h + 1) * hd])
        d3_ref[(3 * h + 2) * hd:(3 * h + 3) * hd] = acc2[h * hd:(h + 1) * hd]


def bwd_attention(me, x_all, dy_all, tab, k_all, v_all, stats, qt, d_ctx_bf, gain, shift, wq, wot, bq, cos_t, sin_t, T, hd, h0, nh):
    S, W = x_all.shape
    heads = W // hd
    width = nh * hd
    cols = slice(h0 * hd, h0 * hd + width)
    vm = pl.BlockSpec(memory_space=pltpu.VMEM)
    anym = pl.BlockSpec(memory_space=pl.ANY)
    f32, bf = jnp.float32, jnp.bfloat16
    return pl.pallas_call(
        functools.partial(bwd_kernel, hd, S // T, heads, h0, width, stats.shape[0] * T // S),
        out_shape=jax.ShapeDtypeStruct((3 * width, T), f32),
        in_specs=[pl.BlockSpec(memory_space=pltpu.SMEM)] + [anym] * 4 + [vm] * 14,
        out_specs=vm,
        scratch_shapes=[pltpu.VMEM((4, T, W), bf), pltpu.VMEM((4, T, W), bf), pltpu.VMEM((T, 128), f32), pltpu.VMEM((T, 128), f32),
                        pltpu.VMEM((4, T, width), bf), pltpu.VMEM((4, T, width), bf), pltpu.VMEM((T, W), bf),
                        pltpu.VMEM((2, T, width), bf), pltpu.VMEM((2, T, width), bf), pltpu.VMEM((nh, 2 * hd, T), bf), pltpu.VMEM((nh, 2 * hd, T), bf),
                        pltpu.VMEM((4, T, T), f32), pltpu.VMEM((width, T), f32), pltpu.VMEM((width, T), f32),
                        pltpu.SemaphoreType.DMA((4, 2)), pltpu.SemaphoreType.DMA((4, 2))],
        compiler_params=pltpu.CompilerParams(vmem_limit_bytes=VMEM_LIMIT),
        cost_estimate=pl.CostEstimate(flops=100_000_000_000, bytes_accessed=30_000_000, transcendentals=0),
        name="attn_bwd",
    )(me, x_all, dy_all, k_all, v_all, *tab, stats, qt, d_ctx_bf, gain, shift, wq[:, cols], wot[:, cols], bq[:, cols], cos_t, sin_t)


def mlp_kernel(x_ref, dy_ref, g_ref, s_ref, wu_ref, bu_ref, wd_ref, du_ref, dd_ref, db_ref):
    @pl.when(pl.program_id(0) == 0)
    def _():
        du_ref[...] = jnp.zeros_like(du_ref)
        dd_ref[...] = jnp.zeros_like(dd_ref)
        db_ref[...] = jnp.zeros_like(db_ref)

    h = layer_norm(x_ref[...].astype(jnp.float32), g_ref[...], s_ref[...])[0].astype(jnp.bfloat16)
    dy = dy_ref[...]
    act, slope = exact_gelu(mm(h, wu_ref[...]) + bu_ref[...])
    d_up = mm(dy, wd_ref[...]) * slope
    keep = du_ref.shape[0]
    db_ref[...] += jnp.sum(d_up, axis=0, keepdims=True)
    du_ref[...] += mm(d_up.astype(jnp.bfloat16).T, h)[:keep]
    dd_ref[...] += mm(act.astype(jnp.bfloat16).T, dy)[:keep]


def mlp_grads(x_all, dy_all, gain, shift, wu, bu, wd, keep):
    S, W = x_all.shape
    F = wu.shape[1]
    R = 512
    const = lambda j: (0, 0)
    return pl.pallas_call(
        mlp_kernel,
        grid=(S // R,),
        out_shape=[jax.ShapeDtypeStruct((keep, W), jnp.float32)] * 2 + [jax.ShapeDtypeStruct((1, F), jnp.float32)],
        in_specs=[pl.BlockSpec((R, W), lambda j: (j, 0)), pl.BlockSpec((R, W), lambda j: (j, 0)), pl.BlockSpec((1, W), const), pl.BlockSpec((1, W), const),
                  pl.BlockSpec((W, F), const), pl.BlockSpec((1, F), const), pl.BlockSpec((W, F), const)],
        out_specs=[pl.BlockSpec((keep, W), const)] * 2 + [pl.BlockSpec((1, F), const)],
        compiler_params=pltpu.CompilerParams(vmem_limit_bytes=VMEM_LIMIT, dimension_semantics=("arbitrary",)),
        cost_estimate=pl.CostEstimate(flops=20_000_000_000, bytes_accessed=26_000_000, transcendentals=0),
        name="mlp_grads",
    )(x_all, dy_all, gain, shift, wu, bu, wd)


def solution(mesh):
    cp_size = mesh.shape['cp']
    row_spec = P('dp', 'cp', None)
    in_specs = (row_spec, row_spec) + (P(),) * 12
    out_specs = (row_spec, row_spec, P('dp'), P('dp'), P('dp'), P('dp'), P('dp', None, None, None), P('dp', None, None), P('dp', None), P('dp'), P('dp', None), P('dp'), P('dp', None), P('dp'))
    bf, f32 = jnp.bfloat16, jnp.float32

    def local_layer(x_blk, dy_blk, ln1_gain, ln1_bias, ln2_gain, ln2_bias, w_qkv, b_qkv, w_out, b_out, w_up, b_up, w_down, b_down):
        T, W = x_blk.shape[1:]
        heads, hd = w_qkv.shape[1], w_qkv.shape[3]
        FF = w_up.shape[1]
        S = T * cp_size
        me = lax.axis_index('cp')
        me1 = me.astype(jnp.int32).reshape(1)
        row = lambda v: v.reshape(1, -1).astype(f32)

        TN = (((0,), (0,)), ((), ()))
        x_own = x_blk[0]
        dy_own = dy_blk[0]
        dy_bf = dy_own.astype(bf)
        x_all = lax.all_gather(x_own, 'cp', tiled=True)
        dy_all = lax.all_gather(dy_bf, 'cp', tiled=True)

        w_rows = w_qkv.transpose(1, 2, 3, 0)
        wq, wk = (pair_rows(w_rows[:, c]).T for c in (0, 1))
        wv = w_rows[:, 2].reshape(W, W).T
        b_rows = b_qkv.astype(f32)[..., None]
        b3 = jnp.stack([pair_rows(b_rows[:, 0])[:, 0], pair_rows(b_rows[:, 1])[:, 0], b_rows[:, 2].reshape(W)])
        wot = w_out.T
        tab = lane_tables(jnp.arange(T), hd) + lane_tables(jnp.arange(cp_size) * T, hd)
        ang = rope_angles(me * T + jnp.arange(T), hd).T
        cos_o, sin_o = jnp.cos(ang), jnp.sin(ang)

        x_rows = x_own.astype(f32)
        h_attn, x_norm1, inv_std1 = layer_norm(x_rows, ln1_gain, ln1_bias)
        h_attn = h_attn.astype(bf)
        h_mlp, x_norm2, inv_std2 = layer_norm(x_rows, ln2_gain, ln2_bias)
        h_mlp = h_mlp.astype(bf)
        gelu_out, slope = exact_gelu(mm(h_mlp, w_up) + b_up.astype(f32))
        y_part = x_rows + (mm(gelu_out.astype(bf), w_down) + b_down.astype(f32)) + b_out.astype(f32)
        d_up_bf = (mm(dy_bf, w_down, NT) * slope).astype(bf)
        d_h_mlp = mm(d_up_bf, w_up, NT)
        d_ctx = mm(dy_bf, w_out, NT)
        d_ctx_bf = d_ctx.astype(bf)
        dx_mlp, d_ln2_gain, d_ln2_bias = norm_backward(d_h_mlp, x_norm2, inv_std2, ln2_gain)
        dx_part = dy_own + dx_mlp
        dy_sum = jnp.sum(dy_own, axis=0)
        F = FF // cp_size
        F_pad = -(-F // 128) * 128
        pad = lambda a, ax: jnp.pad(a, [(0, F_pad - F) if d == ax else (0, 0) for d in range(a.ndim)])
        wu_s = pad(lax.dynamic_slice_in_dim(w_up, me * F, F, 1), 1)
        bu_s = pad(lax.dynamic_slice_in_dim(b_up.astype(f32), me * F, F, 0), 0).reshape(1, F_pad)
        wd_s = pad(lax.dynamic_slice_in_dim(w_down, me * F, F, 0).T, 1)

        (x_in, y_part, dx_part, d_ln2_gain, d_ln2_bias, dy_sum, d_ctx, d_ctx_bf, h_attn, wq, wk, wv, wot, wu_s, wd_s) = lax.optimization_barrier(
            (x_all, y_part, dx_part, d_ln2_gain, d_ln2_bias, dy_sum, d_ctx, d_ctx_bf, h_attn, wq, wk, wv, wot, wu_s, wd_s))
        k_all, v_all, attn_norm, lse, qt = fwd_attention(me1, x_in, tab, row(ln1_gain), row(ln1_bias), wq, wk, wv, b3, T, hd)
        delta = jnp.sum((d_ctx * attn_norm).reshape(T, heads, hd), axis=-1).T
        fill = jnp.zeros((2 * heads, T), f32)
        stats = lax.all_gather(jnp.concatenate([lse, delta, fill], axis=0), 'cp', tiled=True)
        attn_ctx = attn_norm.astype(bf)
        y_rows = (y_part + mm(attn_ctx, w_out)).astype(bf)
        d_w_out = mm(attn_ctx, dy_bf, TN)

        dy_in, _ = lax.optimization_barrier((dy_all, lse))
        du_s, dd_s, db_s = mlp_grads(x_in, dy_in, row(ln2_gain), row(ln2_bias), wu_s, bu_s, wd_s, F)
        d_b_up = lax.dynamic_update_slice(jnp.zeros((FF,), f32), db_s[0, :F], (me * F,))

        stats, y_rows, d_w_out, du_s, dd_s = lax.optimization_barrier((stats, y_rows, d_w_out, du_s, dd_s))
        d_w_up = lax.all_gather(du_s, 'cp', tiled=True)
        d_w_down = lax.all_gather(dd_s, 'cp', tiled=True)
        d3 = bwd_attention(me1, x_in, dy_in, tab, k_all, v_all, stats, qt, d_ctx_bf, row(ln1_gain), row(ln1_bias), wq, wot, b3[0:1], cos_o, sin_o, T, hd, 0, heads)
        d3, d_w_up, d_w_down = lax.optimization_barrier((d3, d_w_up, d_w_down))
        d3_bf = d3.astype(bf)
        d_h = mm(d3_bf, w_rows.reshape(3 * W, W), TN)
        d_w_rows = mm(d3_bf, h_attn)
        dx_attn, d_ln1_gain, d_ln1_bias = norm_backward(d_h, x_norm1, inv_std1, ln1_gain)
        dx_rows = dx_part + dx_attn
        small = jnp.concatenate([d_ln1_gain, d_ln1_bias, d_ln2_gain, d_ln2_bias, dy_sum, jnp.sum(d3, axis=1), d_b_up]).reshape(-1, W)
        d_w_rows, tail = lax.psum((d_w_rows, jnp.concatenate([d_w_out, small], axis=0)), 'cp')
        d_w_out = tail[:W]
        small = tail[W:].reshape(-1)
        d_w_qkv = d_w_rows.reshape(heads, 3, hd, W).transpose(3, 0, 1, 2)
        vec = [small[i * W:(i + 1) * W] for i in range(5)]
        d_b_qkv = small[5 * W:8 * W].reshape(heads, 3, hd)
        d_b_up = small[8 * W:]
        return (y_rows[None], dx_rows[None], vec[0], vec[1], vec[2], vec[3], d_w_qkv, d_b_qkv, d_w_out, vec[4], d_w_up.T, d_b_up, d_w_down, vec[4])

    return jax.shard_map(local_layer, mesh=mesh, in_specs=in_specs, out_specs=out_specs, check_vma=False)
```

```python
import functools

import jax
import jax.numpy as jnp
from jax import lax
from jax.experimental import pallas as pl
from jax.experimental.pallas import tpu as pltpu
from jax.sharding import PartitionSpec as P

EPS = 1e-5
ROPE_BASE = 10000.0
NEG_BIG = -1e30
VMEM_LIMIT = 60 * 1024 * 1024
NN = (((1,), (0,)), ((), ()))
NT = (((1,), (1,)), ((), ()))


def mm(a, b, dims=NN):
    return lax.dot_general(a, b, dims, preferred_element_type=jnp.float32)


def layer_norm(row_vals, norm_gain, norm_shift):
    row_mean = jnp.mean(row_vals, axis=-1, keepdims=True)
    centered = row_vals - row_mean
    inv_std = lax.rsqrt(jnp.mean(centered * centered, axis=-1, keepdims=True) + EPS)
    x_norm = centered * inv_std
    return x_norm * norm_gain + norm_shift, x_norm, inv_std


def norm_backward(d_out, x_norm, inv_std, norm_gain):
    d_norm = d_out * norm_gain
    d_rows = inv_std * (d_norm - jnp.mean(d_norm, axis=-1, keepdims=True) - x_norm * jnp.mean(d_norm * x_norm, axis=-1, keepdims=True))
    return d_rows, jnp.sum(d_out * x_norm, axis=0), jnp.sum(d_out, axis=0)


def rope_angles(positions, head_dim):
    rot_dim = head_dim // 4
    inv_freq = ROPE_BASE ** (-2.0 * jnp.arange(rot_dim // 2, dtype=jnp.float32) / rot_dim)
    return positions.astype(jnp.float32)[:, None] * inv_freq[None, :]


def lane_tables(positions, head_dim):
    rot_dim = head_dim // 4
    freq = ROPE_BASE ** (-2.0 * jnp.arange(rot_dim // 2, dtype=jnp.float32) / rot_dim)
    rest = jnp.zeros((head_dim // 2 - rot_dim // 2,), jnp.float32)
    lanes = jnp.concatenate([-freq, rest, -freq, rest, freq, rest, freq, rest])
    angles = positions.astype(jnp.float32)[:, None] * lanes[None, :]
    return jnp.cos(angles), jnp.sin(angles)


def turn(tab, j, cs, ss):
    cl, sl, cb, sb = tab
    ca, sa = cb[pl.ds(j, 1), :], sb[pl.ds(j, 1), :]
    cs[...] = ca * cl[...] - sa * sl[...]
    ss[...] = sa * cl[...] + ca * sl[...]


def pair_rows(w_t):
    heads, hd = w_t.shape[:2]
    half = hd // 8
    mid = (hd - 2 * half) // 2 + 2 * half
    low = jnp.concatenate([w_t[:, :half], w_t[:, 2 * half:mid]], axis=1)
    high = jnp.concatenate([w_t[:, half:2 * half], w_t[:, mid:]], axis=1)
    both = jnp.stack([low, high], axis=1).reshape(heads // 2, 2, 2, hd // 2, -1)
    return both.transpose(0, 2, 1, 3, 4).reshape(heads * hd, -1)


def rotate(z, cos_l, sin_l):
    parts = []
    for t in range(z.shape[1] // 128):
        zt = z[:, t * 128:(t + 1) * 128]
        parts.append(zt * cos_l + pltpu.roll(zt, 64, 1) * sin_l)
    return jnp.concatenate(parts, axis=1)


def exact_gelu(pre):
    cdf = 0.5 * (1.0 + lax.erf(pre * (0.5 ** 0.5)))
    pdf = jnp.exp(-0.5 * pre * pre) * 0.3989422804014327
    return pre * cdf, cdf + pre * pdf


def put_masked(dst, mat_t, hd, paired):
    rows = lax.broadcasted_iota(jnp.int32, (2 * hd, mat_t.shape[1]), 0)
    first = (rows % hd < hd // 2) if paired else (rows < hd)
    for p in range(mat_t.shape[0] // (2 * hd)):
        blk = mat_t[p * 2 * hd:(p + 1) * 2 * hd]
        zero = jnp.zeros_like(blk)
        dst[2 * p] = jnp.where(first, blk, zero)
        dst[2 * p + 1] = jnp.where(first, zero, blk)


def head_rows(mat_t, i, hd, paired):
    if not paired:
        return mat_t[i * hd:(i + 1) * hd]
    q = hd // 2
    return jnp.concatenate([mat_t[i * q:(i + 1) * q], mat_t[hd + i * q:hd + (i + 1) * q]], axis=0)


def causal(T, keys_first):
    r = lax.broadcasted_iota(jnp.int32, (T, T), 0)
    c = lax.broadcasted_iota(jnp.int32, (T, T), 1)
    return (r <= c) if keys_first else (c <= r)


def fwd_kernel(hd, me_ref, x_hbm, cl_ref, sl_ref, cb_ref, sb_ref, g_ref, s_ref, wq_ref, wk_ref, wv_ref, b_ref,
               k_hbm, v_hbm, ctx_ref, lse_ref, qt_ref,
               xb, cs, ss, hsc, kst, vst, qtm, sbuf, acc, mrow, lrow, in_sem, out_sem):
    me = me_ref[0]
    T = xb.shape[1]
    W = xb.shape[2]
    pairs = W // (2 * hd)
    scale = hd ** -0.5
    tiles = W // 256

    tab = (cl_ref, sl_ref, cb_ref, sb_ref)
    DEEP = xb.shape[0]

    def fetch(j):
        blk = jnp.where(j < 0, me, jnp.minimum(j, me))
        slot = (j + 1) % DEEP
        return (pltpu.make_async_copy(x_hbm.at[pl.ds(blk * T, T)], xb.at[slot], in_sem.at[slot]),)

    def flush(j, slot):
        return (pltpu.make_async_copy(kst.at[slot], k_hbm.at[pl.ds(j * T, T)], out_sem.at[slot, 0]),
                pltpu.make_async_copy(vst.at[slot], v_hbm.at[pl.ds(j * T, T)], out_sem.at[slot, 1]))

    def start(copies):
        for c in copies:
            c.start()

    def wait(copies):
        for c in copies:
            c.wait()

    def norm(j):
        hsc[...] = layer_norm(xb[(j + 1) % DEEP].astype(jnp.float32), g_ref[...], s_ref[...])[0].astype(jnp.bfloat16)
        turn(tab, jnp.where(j < 0, me, j), cs, ss)

    def project(slot):
        kst[slot] = rotate(mm(hsc[...], wk_ref[...]) + b_ref[1:2], cs[...], ss[...]).astype(jnp.bfloat16)
        vst[slot] = (mm(hsc[...], wv_ref[...]) + b_ref[2:3]).astype(jnp.bfloat16)

    def scores(slot, h):
        return mm(kst[slot, :, h // 2 * 2 * hd:(h // 2 + 1) * 2 * hd], qtm[h])

    def attend(j, slot, diag):
        ahead = [scores(slot, 0), scores(slot, 1)] if diag else [sbuf[0], sbuf[1]]
        norm(j + 1)
        project(1 - slot)
        for p in range(pairs):
            now = ahead
            ahead = [scores(slot, 2 * p + 2 + i) if p + 1 < pairs else scores(1 - slot, i) for i in range(2)]
            vt = vst[slot, :, p * 2 * hd:(p + 1) * 2 * hd].T
            for i in range(2):
                h = 2 * p + i
                s = now[i]
                rows = slice(h * hd, (h + 1) * hd)
                vh = head_rows(vt, i, hd, False)
                if diag:
                    s = jnp.where(causal(T, True), s, NEG_BIG)
                    m = jnp.max(s, axis=0, keepdims=True)
                    e = jnp.exp(s - m)
                    lrow[h:h + 1] = jnp.sum(e, axis=0, keepdims=True)
                    acc[rows] = mm(vh, e.astype(jnp.bfloat16))
                else:
                    m_old = mrow[h:h + 1]
                    m = jnp.maximum(m_old, jnp.max(s, axis=0, keepdims=True))
                    e = jnp.exp(s - m)
                    alpha = jnp.exp(m_old - m)
                    lrow[h:h + 1] = lrow[h:h + 1] * alpha + jnp.sum(e, axis=0, keepdims=True)
                    acc[rows] = acc[rows] * alpha + mm(vh, e.astype(jnp.bfloat16))
                mrow[h:h + 1] = m
        sbuf[0], sbuf[1] = ahead

    for j in range(-1, DEEP - 1):
        start(fetch(jnp.int32(j)))
    own = jnp.int32(-1)
    wait(fetch(own))
    norm(own)
    project(0)
    for t in range(tiles):
        cols = slice(t * 256, (t + 1) * 256)
        q = rotate(mm(hsc[...], wq_ref[:, cols]) + b_ref[0:1, cols], cs[...], ss[...])
        qt_ref[cols] = (q.astype(jnp.bfloat16) * jnp.bfloat16(scale)).T
    put_masked(qtm, qt_ref[...], hd, True)
    start(flush(me, 0))
    start(fetch(own + DEEP))
    wait(fetch(own + 1))
    attend(own, 0, True)

    @pl.when(me >= 1)
    def _():
        start(flush(0, 1))

    wait(flush(me, 0))

    def step(j, slot):
        wait(fetch(j + 1))
        start(fetch(j + DEEP))

        @pl.when(j >= 1)
        def _():
            wait(flush(j - 1, 1 - slot))

        attend(j, slot, False)

        @pl.when(j + 1 < me)
        def _():
            start(flush(j + 1, 1 - slot))

        return 1 - slot

    last = lax.fori_loop(0, me, step, jnp.int32(1))

    for k in range(1, DEEP):
        wait(fetch(me + k))

    @pl.when(me >= 1)
    def _():
        wait(flush(me - 1, 1 - last))

    lse_ref[...] = mrow[...] + jnp.log(lrow[...])
    inv = 1.0 / lrow[...]
    for p in range(pairs):
        a = acc[2 * p * hd:(2 * p + 1) * hd] * inv[2 * p:2 * p + 1]
        b = acc[(2 * p + 1) * hd:(2 * p + 2) * hd] * inv[2 * p + 1:2 * p + 2]
        ctx_ref[:, 2 * p * hd:(2 * p + 2) * hd] = jnp.concatenate([a, b], axis=0).T


def fwd_attention(me, x_all, tab, gain, shift, wq, wk, wv, b3, T, hd):
    S, W = x_all.shape
    heads = W // hd
    vm = pl.BlockSpec(memory_space=pltpu.VMEM)
    anym = pl.BlockSpec(memory_space=pl.ANY)
    f32, bf = jnp.float32, jnp.bfloat16
    return pl.pallas_call(
        functools.partial(fwd_kernel, hd),
        out_shape=[jax.ShapeDtypeStruct((S, W), bf), jax.ShapeDtypeStruct((S, W), bf), jax.ShapeDtypeStruct((T, W), f32),
                   jax.ShapeDtypeStruct((heads, T), f32), jax.ShapeDtypeStruct((W, T), bf)],
        in_specs=[pl.BlockSpec(memory_space=pltpu.SMEM), anym] + [vm] * 10,
        out_specs=[anym, anym, vm, vm, vm],
        scratch_shapes=[pltpu.VMEM((4, T, W), bf), pltpu.VMEM((T, 128), f32), pltpu.VMEM((T, 128), f32), pltpu.VMEM((T, W), bf),
                        pltpu.VMEM((2, T, W), bf), pltpu.VMEM((2, T, W), bf), pltpu.VMEM((heads, 2 * hd, T), bf), pltpu.VMEM((2, T, T), f32),
                        pltpu.VMEM((W, T), f32), pltpu.VMEM((heads, T), f32), pltpu.VMEM((heads, T), f32),
                        pltpu.SemaphoreType.DMA((4,)), pltpu.SemaphoreType.DMA((2, 2))],
        compiler_params=pltpu.CompilerParams(vmem_limit_bytes=VMEM_LIMIT),
        cost_estimate=pl.CostEstimate(flops=40_000_000_000, bytes_accessed=40_000_000, transcendentals=0),
        name="attn_fwd",
    )(me, x_all, *tab, gain, shift, wq, wk, wv, b3)


def proj_kernel(hd, n, me_ref, x_hbm, dy_hbm, cl_ref, sl_ref, cb_ref, sb_ref, g_ref, s_ref, wq_ref, wot_ref, bq_ref, q_hbm, o_hbm,
                xb, yb, cs, ss, hsc, qst, ost, in_sem, out_sem):
    me = me_ref[0]
    DEEP, T, W = xb.shape
    scale = hd ** -0.5
    tab = (cl_ref, sl_ref, cb_ref, sb_ref)

    def fetch(r):
        slot, blk = r % DEEP, jnp.minimum(me + r, n - 1)
        return (pltpu.make_async_copy(x_hbm.at[pl.ds(blk * T, T)], xb.at[slot], in_sem.at[slot, 0]),
                pltpu.make_async_copy(dy_hbm.at[pl.ds(blk * T, T)], yb.at[slot], in_sem.at[slot, 1]))

    def flush(r):
        slot = r % 2
        return (pltpu.make_async_copy(qst.at[slot], q_hbm.at[pl.ds((me + r) * T, T)], out_sem.at[slot, 0]),
                pltpu.make_async_copy(ost.at[slot], o_hbm.at[pl.ds((me + r) * T, T)], out_sem.at[slot, 1]))

    def start(copies):
        for c in copies:
            c.start()

    def wait(copies):
        for c in copies:
            c.wait()

    for r in range(DEEP - 1):
        start(fetch(jnp.int32(r)))

    def step(r, _):
        start(fetch(r + DEEP - 1))
        wait(fetch(r))

        @pl.when(r >= 2)
        def _():
            wait(flush(r - 2))

        turn(tab, me + r, cs, ss)
        for t in range(W // 256):
            cols = slice(t * 256, (t + 1) * 256)
            ost[r % 2, :, cols] = mm(yb[r % DEEP], wot_ref[:, cols]).astype(jnp.bfloat16)
        hsc[...] = layer_norm(xb[r % DEEP].astype(jnp.float32), g_ref[...], s_ref[...])[0].astype(jnp.bfloat16)
        for t in range(W // 256):
            cols = slice(t * 256, (t + 1) * 256)
            q = rotate(mm(hsc[...], wq_ref[:, cols]) + bq_ref[:, cols], cs[...], ss[...])
            qst[r % 2, :, cols] = q.astype(jnp.bfloat16) * jnp.bfloat16(scale)
        start(flush(r))
        return 0

    count = n - me
    lax.fori_loop(0, count, step, 0)
    for k in range(DEEP - 1):
        wait(fetch(count + k))
    wait(flush(count - 1))

    @pl.when(count >= 2)
    def _():
        wait(flush(count - 2))


def later_blocks(me, x_all, dy_all, tab, gain, shift, wq, wot, bq, T, hd):
    S, W = x_all.shape
    vm = pl.BlockSpec(memory_space=pltpu.VMEM)
    anym = pl.BlockSpec(memory_space=pl.ANY)
    f32, bf = jnp.float32, jnp.bfloat16
    return pl.pallas_call(
        functools.partial(proj_kernel, hd, S // T),
        out_shape=[jax.ShapeDtypeStruct((S, W), bf)] * 2,
        in_specs=[pl.BlockSpec(memory_space=pltpu.SMEM), anym, anym] + [vm] * 9,
        out_specs=[anym, anym],
        scratch_shapes=[pltpu.VMEM((4, T, W), bf), pltpu.VMEM((4, T, W), bf), pltpu.VMEM((T, 128), f32), pltpu.VMEM((T, 128), f32), pltpu.VMEM((T, W), bf),
                        pltpu.VMEM((2, T, W), bf), pltpu.VMEM((2, T, W), bf), pltpu.SemaphoreType.DMA((4, 2)), pltpu.SemaphoreType.DMA((2, 2))],
        compiler_params=pltpu.CompilerParams(vmem_limit_bytes=VMEM_LIMIT),
        cost_estimate=pl.CostEstimate(flops=20_000_000_000, bytes_accessed=40_000_000, transcendentals=0),
        name="later_blocks",
    )(me, x_all, dy_all, *tab, gain, shift, wq, wot, bq)


def bwd_kernel(hd, n, srows, me_ref, k_hbm, v_hbm, q_hbm, o_hbm, stats_ref, qt_ref, own_ref, ct_ref, st_ref, d3_ref,
               kb, vb, qb, ob, am, bm, sbuf, acc1, acc2, kv_sem, qo_sem):
    me = me_ref[0]
    DEEP, T, W = kb.shape
    heads = W // hd
    half = hd // 8
    scale = hd ** -0.5

    def fetch_kv(j):
        slot, blk = j % DEEP, jnp.minimum(j, me)
        return (pltpu.make_async_copy(k_hbm.at[pl.ds(blk * T, T)], kb.at[slot], kv_sem.at[slot, 0]),
                pltpu.make_async_copy(v_hbm.at[pl.ds(blk * T, T)], vb.at[slot], kv_sem.at[slot, 1]))

    def fetch_qo(r):
        slot, blk = r % DEEP, jnp.minimum(me + r, n - 1)
        return (pltpu.make_async_copy(q_hbm.at[pl.ds(blk * T, T)], qb.at[slot], qo_sem.at[slot, 0]),
                pltpu.make_async_copy(o_hbm.at[pl.ds(blk * T, T)], ob.at[slot], qo_sem.at[slot, 1]))

    def start(copies):
        for c in copies:
            c.start()

    def wait(copies):
        for c in copies:
            c.wait()

    def pair_cols(h):
        return slice(h // 2 * 2 * hd, (h // 2 + 1) * 2 * hd)

    def unrotated(z):
        mid = hd // 2
        a, b = z[:half], z[mid:mid + half]
        ct, st = ct_ref[...], st_ref[...]
        return jnp.concatenate([a * ct + b * st, b * ct - a * st, z[half:mid], z[mid + half:]], axis=0)

    def two_scores(left, right, slot, h):
        return mm(left[slot, :, pair_cols(h)], am[h]), mm(right[slot, :, pair_cols(h)], bm[h])

    for r in range(DEEP - 1):
        start(fetch_kv(jnp.int32(r)))
        start(fetch_qo(jnp.int32(r)))
    put_masked(am, qt_ref[...], hd, True)
    put_masked(bm, own_ref[...].T, hd, False)
    acc1[...] = jnp.zeros_like(acc1)
    zero = jnp.int32(0)

    def dq_block(j, diag):
        slot = j % DEEP
        ahead = [(sbuf[0], sbuf[1]), (sbuf[2], sbuf[3])]
        for h in range(heads):
            s, dp = ahead.pop(0)
            ahead.append(two_scores(kb, vb, slot, h + 2) if h + 2 < heads else two_scores(kb, vb, (j + 1) % DEEP, h + 2 - heads))
            if h % 2 == 0:
                kt = kb[slot, :, pair_cols(h)].T
            if diag:
                s = jnp.where(causal(T, True), s, NEG_BIG)
            pr = jnp.exp(s - stats_ref[pl.ds(me * srows + h, 1), :])
            ds = (pr * (dp - stats_ref[pl.ds(me * srows + heads + h, 1), :])).astype(jnp.bfloat16)
            acc1[h * hd:(h + 1) * hd] += mm(head_rows(kt, h % 2, hd, True), ds)
        (sbuf[0], sbuf[1]), (sbuf[2], sbuf[3]) = ahead

    wait(fetch_kv(zero))
    sbuf[0], sbuf[1] = two_scores(kb, vb, 0, 0)
    sbuf[2], sbuf[3] = two_scores(kb, vb, 0, 1)

    def dq_step(j, _):
        start(fetch_kv(j + DEEP - 1))
        wait(fetch_kv(j + 1))
        dq_block(j, False)
        return 0

    lax.fori_loop(0, me, dq_step, 0)
    for k in range(1, DEEP - 1):
        wait(fetch_kv(me + k))
    dq_block(me, True)
    last = me % DEEP
    for h in range(heads):
        d3_ref[3 * h * hd:(3 * h + 1) * hd] = unrotated(acc1[h * hd:(h + 1) * hd] * scale)

    put_masked(am, kb[last].T, hd, True)
    put_masked(bm, vb[last].T, hd, False)
    acc1[...] = jnp.zeros_like(acc1)
    acc2[...] = jnp.zeros_like(acc2)

    def dkv_block(r, diag):
        slot = r % DEEP
        ahead = [(sbuf[0], sbuf[1]), (sbuf[2], sbuf[3])]
        stc = stats_ref[pl.ds((me + r) * srows, 2 * heads), :].T
        for h in range(heads):
            s, dp = ahead.pop(0)
            ahead.append(two_scores(qb, ob, slot, h + 2) if h + 2 < heads else two_scores(qb, ob, (r + 1) % DEEP, h + 2 - heads))
            if h % 2 == 0:
                qt = qb[slot, :, pair_cols(h)].T
                ot = ob[slot, :, pair_cols(h)].T
            if diag:
                s = jnp.where(causal(T, False), s, NEG_BIG)
            rows = slice(h * hd, (h + 1) * hd)
            pr = jnp.exp(s - stc[:, h:h + 1])
            acc2[rows] += mm(head_rows(ot, h % 2, hd, False), pr.astype(jnp.bfloat16))
            ds = (pr * (dp - stc[:, heads + h:heads + h + 1])).astype(jnp.bfloat16)
            acc1[rows] += mm(head_rows(qt, h % 2, hd, True), ds)
        (sbuf[0], sbuf[1]), (sbuf[2], sbuf[3]) = ahead

    wait(fetch_qo(zero))
    sbuf[0], sbuf[1] = two_scores(qb, ob, 0, 0)
    sbuf[2], sbuf[3] = two_scores(qb, ob, 0, 1)

    def dkv_step(r, diag):
        start(fetch_qo(r + DEEP - 1))
        wait(fetch_qo(r + 1))
        dkv_block(r, diag)
        return 0

    dkv_step(zero, True)
    lax.fori_loop(1, n - me, lambda r, _: dkv_step(r, False), 0)
    for k in range(1, DEEP - 1):
        wait(fetch_qo(n - me + k))
    for h in range(heads):
        d3_ref[(3 * h + 1) * hd:(3 * h + 2) * hd] = unrotated(acc1[h * hd:(h + 1) * hd])
        d3_ref[(3 * h + 2) * hd:(3 * h + 3) * hd] = acc2[h * hd:(h + 1) * hd]


def bwd_attention(me, k_all, v_all, q_all, o_all, stats, qt, d_ctx_bf, cos_t, sin_t, T, hd):
    S, W = k_all.shape
    heads = W // hd
    vm = pl.BlockSpec(memory_space=pltpu.VMEM)
    anym = pl.BlockSpec(memory_space=pl.ANY)
    f32, bf = jnp.float32, jnp.bfloat16
    return pl.pallas_call(
        functools.partial(bwd_kernel, hd, S // T, stats.shape[0] * T // S),
        out_shape=jax.ShapeDtypeStruct((3 * W, T), f32),
        in_specs=[pl.BlockSpec(memory_space=pltpu.SMEM)] + [anym] * 4 + [vm] * 5,
        out_specs=vm,
        scratch_shapes=[pltpu.VMEM((4, T, W), bf)] * 4 + [pltpu.VMEM((heads, 2 * hd, T), bf), pltpu.VMEM((heads, 2 * hd, T), bf),
                        pltpu.VMEM((4, T, T), f32), pltpu.VMEM((W, T), f32), pltpu.VMEM((W, T), f32),
                        pltpu.SemaphoreType.DMA((4, 2)), pltpu.SemaphoreType.DMA((4, 2))],
        compiler_params=pltpu.CompilerParams(vmem_limit_bytes=VMEM_LIMIT),
        cost_estimate=pl.CostEstimate(flops=100_000_000_000, bytes_accessed=30_000_000, transcendentals=0),
        name="attn_bwd",
    )(me, k_all, v_all, q_all, o_all, stats, qt, d_ctx_bf, cos_t, sin_t)


def mlp_kernel(x_ref, dy_ref, g_ref, s_ref, wu_ref, bu_ref, wd_ref, du_ref, dd_ref, db_ref):
    @pl.when(pl.program_id(0) == 0)
    def _():
        du_ref[...] = jnp.zeros_like(du_ref)
        dd_ref[...] = jnp.zeros_like(dd_ref)
        db_ref[...] = jnp.zeros_like(db_ref)

    h = layer_norm(x_ref[...].astype(jnp.float32), g_ref[...], s_ref[...])[0].astype(jnp.bfloat16)
    dy = dy_ref[...]
    act, slope = exact_gelu(mm(h, wu_ref[...]) + bu_ref[...])
    d_up = mm(dy, wd_ref[...]) * slope
    keep = du_ref.shape[0]
    db_ref[...] += jnp.sum(d_up, axis=0, keepdims=True)
    du_ref[...] += mm(d_up.astype(jnp.bfloat16).T, h)[:keep]
    dd_ref[...] += mm(act.astype(jnp.bfloat16).T, dy)[:keep]


def mlp_grads(x_all, dy_all, gain, shift, wu, bu, wd, keep):
    S, W = x_all.shape
    F = wu.shape[1]
    R = 512
    const = lambda j: (0, 0)
    return pl.pallas_call(
        mlp_kernel,
        grid=(S // R,),
        out_shape=[jax.ShapeDtypeStruct((keep, W), jnp.float32)] * 2 + [jax.ShapeDtypeStruct((1, F), jnp.float32)],
        in_specs=[pl.BlockSpec((R, W), lambda j: (j, 0)), pl.BlockSpec((R, W), lambda j: (j, 0)), pl.BlockSpec((1, W), const), pl.BlockSpec((1, W), const),
                  pl.BlockSpec((W, F), const), pl.BlockSpec((1, F), const), pl.BlockSpec((W, F), const)],
        out_specs=[pl.BlockSpec((keep, W), const)] * 2 + [pl.BlockSpec((1, F), const)],
        compiler_params=pltpu.CompilerParams(vmem_limit_bytes=VMEM_LIMIT, dimension_semantics=("arbitrary",)),
        cost_estimate=pl.CostEstimate(flops=20_000_000_000, bytes_accessed=26_000_000, transcendentals=0),
        name="mlp_grads",
    )(x_all, dy_all, gain, shift, wu, bu, wd)


def solution(mesh):
    cp_size = mesh.shape['cp']
    row_spec = P('dp', 'cp', None)
    in_specs = (row_spec, row_spec) + (P(),) * 12
    out_specs = (row_spec, row_spec, P('dp'), P('dp'), P('dp'), P('dp'), P('dp', None, None, None), P('dp', None, None), P('dp', None), P('dp'), P('dp', None), P('dp'), P('dp', None), P('dp'))
    bf, f32 = jnp.bfloat16, jnp.float32

    def local_layer(x_blk, dy_blk, ln1_gain, ln1_bias, ln2_gain, ln2_bias, w_qkv, b_qkv, w_out, b_out, w_up, b_up, w_down, b_down):
        T, W = x_blk.shape[1:]
        heads, hd = w_qkv.shape[1], w_qkv.shape[3]
        FF = w_up.shape[1]
        S = T * cp_size
        me = lax.axis_index('cp')
        me1 = me.astype(jnp.int32).reshape(1)
        row = lambda v: v.reshape(1, -1).astype(f32)

        TN = (((0,), (0,)), ((), ()))
        x_own = x_blk[0]
        dy_own = dy_blk[0]
        dy_bf = dy_own.astype(bf)
        x_all = lax.all_gather(x_own, 'cp', tiled=True)
        dy_all = lax.all_gather(dy_bf, 'cp', tiled=True)

        w_rows = w_qkv.transpose(1, 2, 3, 0)
        wq, wk = (pair_rows(w_rows[:, c]).T for c in (0, 1))
        wv = w_rows[:, 2].reshape(W, W).T
        b_rows = b_qkv.astype(f32)[..., None]
        b3 = jnp.stack([pair_rows(b_rows[:, 0])[:, 0], pair_rows(b_rows[:, 1])[:, 0], b_rows[:, 2].reshape(W)])
        wot = w_out.T
        tab = lane_tables(jnp.arange(T), hd) + lane_tables(jnp.arange(cp_size) * T, hd)
        ang = rope_angles(me * T + jnp.arange(T), hd).T
        cos_o, sin_o = jnp.cos(ang), jnp.sin(ang)

        x_rows = x_own.astype(f32)
        h_attn, x_norm1, inv_std1 = layer_norm(x_rows, ln1_gain, ln1_bias)
        h_attn = h_attn.astype(bf)
        h_mlp, x_norm2, inv_std2 = layer_norm(x_rows, ln2_gain, ln2_bias)
        h_mlp = h_mlp.astype(bf)
        gelu_out, slope = exact_gelu(mm(h_mlp, w_up) + b_up.astype(f32))
        y_part = x_rows + (mm(gelu_out.astype(bf), w_down) + b_down.astype(f32)) + b_out.astype(f32)
        d_up_bf = (mm(dy_bf, w_down, NT) * slope).astype(bf)
        d_h_mlp = mm(d_up_bf, w_up, NT)
        d_ctx = mm(dy_bf, w_out, NT)
        d_ctx_bf = d_ctx.astype(bf)
        dx_mlp, d_ln2_gain, d_ln2_bias = norm_backward(d_h_mlp, x_norm2, inv_std2, ln2_gain)
        dx_part = dy_own + dx_mlp
        dy_sum = jnp.sum(dy_own, axis=0)
        F = FF // cp_size
        F_pad = -(-F // 128) * 128
        pad = lambda a, ax: jnp.pad(a, [(0, F_pad - F) if d == ax else (0, 0) for d in range(a.ndim)])
        wu_s = pad(lax.dynamic_slice_in_dim(w_up, me * F, F, 1), 1)
        bu_s = pad(lax.dynamic_slice_in_dim(b_up.astype(f32), me * F, F, 0), 0).reshape(1, F_pad)
        wd_s = pad(lax.dynamic_slice_in_dim(w_down, me * F, F, 0).T, 1)

        (x_in, y_part, dx_part, d_ln2_gain, d_ln2_bias, dy_sum, d_ctx, d_ctx_bf, h_attn, wq, wk, wv, wot, wu_s, wd_s) = lax.optimization_barrier(
            (x_all, y_part, dx_part, d_ln2_gain, d_ln2_bias, dy_sum, d_ctx, d_ctx_bf, h_attn, wq, wk, wv, wot, wu_s, wd_s))
        k_all, v_all, attn_norm, lse, qt = fwd_attention(me1, x_in, tab, row(ln1_gain), row(ln1_bias), wq, wk, wv, b3, T, hd)
        delta = jnp.sum((d_ctx * attn_norm).reshape(T, heads, hd), axis=-1).T
        fill = jnp.zeros((2 * heads, T), f32)
        stats = lax.all_gather(jnp.concatenate([lse, delta, fill], axis=0), 'cp', tiled=True)
        attn_ctx = attn_norm.astype(bf)
        y_rows = (y_part + mm(attn_ctx, w_out)).astype(bf)
        d_w_out = mm(attn_ctx, dy_bf, TN)

        dy_in, _ = lax.optimization_barrier((dy_all, lse))
        du_s, dd_s, db_s = mlp_grads(x_in, dy_in, row(ln2_gain), row(ln2_bias), wu_s, bu_s, wd_s, F)
        d_b_up = lax.dynamic_update_slice(jnp.zeros((FF,), f32), db_s[0, :F], (me * F,))

        q_all, o_all = later_blocks(me1, x_in, dy_in, tab, row(ln1_gain), row(ln1_bias), wq, wot, b3[0:1], T, hd)
        stats, d_w_out, du_s, dd_s, q_all = lax.optimization_barrier((stats, d_w_out, du_s, dd_s, q_all))
        d_w_up = lax.all_gather(du_s, 'cp', tiled=True)
        d_w_down = lax.all_gather(dd_s, 'cp', tiled=True)
        d3 = bwd_attention(me1, k_all, v_all, q_all, o_all, stats, qt, d_ctx_bf, cos_o, sin_o, T, hd)
        d3, d_w_up, d_w_down = lax.optimization_barrier((d3, d_w_up, d_w_down))
        d3_bf = d3.astype(bf)
        d_h = mm(d3_bf, w_rows.reshape(3 * W, W), TN)
        d_w_rows = mm(d3_bf, h_attn)
        dx_attn, d_ln1_gain, d_ln1_bias = norm_backward(d_h, x_norm1, inv_std1, ln1_gain)
        dx_rows = dx_part + dx_attn
        small = jnp.concatenate([d_ln1_gain, d_ln1_bias, d_ln2_gain, d_ln2_bias, dy_sum, jnp.sum(d3, axis=1), d_b_up]).reshape(-1, W)
        d_w_rows, tail = lax.psum((d_w_rows, jnp.concatenate([d_w_out, small], axis=0)), 'cp')
        d_w_out = tail[:W]
        small = tail[W:].reshape(-1)
        d_w_qkv = d_w_rows.reshape(heads, 3, hd, W).transpose(3, 0, 1, 2)
        vec = [small[i * W:(i + 1) * W] for i in range(5)]
        d_b_qkv = small[5 * W:8 * W].reshape(heads, 3, hd)
        d_b_up = small[8 * W:]
        return (y_rows[None], dx_rows[None], vec[0], vec[1], vec[2], vec[3], d_w_qkv, d_b_qkv, d_w_out, vec[4], d_w_up.T, d_b_up, d_w_down, vec[4])

    return jax.shard_map(local_layer, mesh=mesh, in_specs=in_specs, out_specs=out_specs, check_vma=False)
```

```python
import functools

import jax
import jax.numpy as jnp
from jax import lax
from jax.experimental import pallas as pl
from jax.experimental.pallas import tpu as pltpu
from jax.sharding import PartitionSpec as P

EPS = 1e-5
ROPE_BASE = 10000.0
NEG_BIG = -1e30
VMEM_LIMIT = 60 * 1024 * 1024
NN = (((1,), (0,)), ((), ()))
NT = (((1,), (1,)), ((), ()))


def mm(a, b, dims=NN):
    return lax.dot_general(a, b, dims, preferred_element_type=jnp.float32)


def layer_norm(row_vals, norm_gain, norm_shift):
    row_mean = jnp.mean(row_vals, axis=-1, keepdims=True)
    centered = row_vals - row_mean
    inv_std = lax.rsqrt(jnp.mean(centered * centered, axis=-1, keepdims=True) + EPS)
    x_norm = centered * inv_std
    return x_norm * norm_gain + norm_shift, x_norm, inv_std


def norm_backward(d_out, x_norm, inv_std, norm_gain):
    d_norm = d_out * norm_gain
    d_rows = inv_std * (d_norm - jnp.mean(d_norm, axis=-1, keepdims=True) - x_norm * jnp.mean(d_norm * x_norm, axis=-1, keepdims=True))
    return d_rows, jnp.sum(d_out * x_norm, axis=0), jnp.sum(d_out, axis=0)


def rope_angles(positions, head_dim):
    rot_dim = head_dim // 4
    inv_freq = ROPE_BASE ** (-2.0 * jnp.arange(rot_dim // 2, dtype=jnp.float32) / rot_dim)
    return positions.astype(jnp.float32)[:, None] * inv_freq[None, :]


def lane_tables(positions, head_dim):
    rot_dim = head_dim // 4
    freq = ROPE_BASE ** (-2.0 * jnp.arange(rot_dim // 2, dtype=jnp.float32) / rot_dim)
    rest = jnp.zeros((head_dim // 2 - rot_dim // 2,), jnp.float32)
    lanes = jnp.concatenate([-freq, rest, -freq, rest, freq, rest, freq, rest])
    angles = positions.astype(jnp.float32)[:, None] * lanes[None, :]
    return jnp.cos(angles), jnp.sin(angles)


def turn(tab, j, cs, ss):
    cl, sl, cb, sb = tab
    ca, sa = cb[pl.ds(j, 1), :], sb[pl.ds(j, 1), :]
    cs[...] = ca * cl[...] - sa * sl[...]
    ss[...] = sa * cl[...] + ca * sl[...]


def pair_rows(w_t):
    heads, hd = w_t.shape[:2]
    half = hd // 8
    mid = (hd - 2 * half) // 2 + 2 * half
    low = jnp.concatenate([w_t[:, :half], w_t[:, 2 * half:mid]], axis=1)
    high = jnp.concatenate([w_t[:, half:2 * half], w_t[:, mid:]], axis=1)
    both = jnp.stack([low, high], axis=1).reshape(heads // 2, 2, 2, hd // 2, -1)
    return both.transpose(0, 2, 1, 3, 4).reshape(heads * hd, -1)


def rotate(z, cos_l, sin_l):
    parts = []
    for t in range(z.shape[1] // 128):
        zt = z[:, t * 128:(t + 1) * 128]
        parts.append(zt * cos_l + pltpu.roll(zt, 64, 1) * sin_l)
    return jnp.concatenate(parts, axis=1)


def exact_gelu(pre):
    cdf = 0.5 * (1.0 + lax.erf(pre * (0.5 ** 0.5)))
    pdf = jnp.exp(-0.5 * pre * pre) * 0.3989422804014327
    return pre * cdf, cdf + pre * pdf


def put_masked(dst, mat_t, hd, paired):
    rows = lax.broadcasted_iota(jnp.int32, (2 * hd, mat_t.shape[1]), 0)
    first = (rows % hd < hd // 2) if paired else (rows < hd)
    for p in range(mat_t.shape[0] // (2 * hd)):
        blk = mat_t[p * 2 * hd:(p + 1) * 2 * hd]
        zero = jnp.zeros_like(blk)
        dst[2 * p] = jnp.where(first, blk, zero)
        dst[2 * p + 1] = jnp.where(first, zero, blk)


def head_rows(mat_t, i, hd, paired):
    if not paired:
        return mat_t[i * hd:(i + 1) * hd]
    q = hd // 2
    return jnp.concatenate([mat_t[i * q:(i + 1) * q], mat_t[hd + i * q:hd + (i + 1) * q]], axis=0)


def causal(T, keys_first):
    r = lax.broadcasted_iota(jnp.int32, (T, T), 0)
    c = lax.broadcasted_iota(jnp.int32, (T, T), 1)
    return (r <= c) if keys_first else (c <= r)


def fwd_kernel(hd, me_ref, x_hbm, cl_ref, sl_ref, cb_ref, sb_ref, g_ref, s_ref, wq_ref, wk_ref, wv_ref, b_ref,
               k_hbm, v_hbm, ctx_ref, lse_ref, qt_ref,
               xb, cs, ss, hsc, kst, vst, qtm, sbuf, acc, mrow, lrow, in_sem, out_sem):
    me = me_ref[0]
    T = xb.shape[1]
    W = xb.shape[2]
    pairs = W // (2 * hd)
    scale = hd ** -0.5
    tiles = W // 256

    tab = (cl_ref, sl_ref, cb_ref, sb_ref)
    DEEP = xb.shape[0]

    def fetch(j):
        blk = jnp.where(j < 0, me, jnp.minimum(j, me))
        slot = (j + 1) % DEEP
        return (pltpu.make_async_copy(x_hbm.at[pl.ds(blk * T, T)], xb.at[slot], in_sem.at[slot]),)

    def flush(j, slot):
        return (pltpu.make_async_copy(kst.at[slot], k_hbm.at[pl.ds(j * T, T)], out_sem.at[slot, 0]),
                pltpu.make_async_copy(vst.at[slot], v_hbm.at[pl.ds(j * T, T)], out_sem.at[slot, 1]))

    def start(copies):
        for c in copies:
            c.start()

    def wait(copies):
        for c in copies:
            c.wait()

    def norm(j):
        hsc[...] = layer_norm(xb[(j + 1) % DEEP].astype(jnp.float32), g_ref[...], s_ref[...])[0].astype(jnp.bfloat16)
        turn(tab, jnp.where(j < 0, me, j), cs, ss)

    def project(slot):
        kst[slot] = rotate(mm(hsc[...], wk_ref[...]) + b_ref[1:2], cs[...], ss[...]).astype(jnp.bfloat16)
        vst[slot] = (mm(hsc[...], wv_ref[...]) + b_ref[2:3]).astype(jnp.bfloat16)

    def scores(slot, h):
        return mm(kst[slot, :, h // 2 * 2 * hd:(h // 2 + 1) * 2 * hd], qtm[h])

    def attend(j, slot, diag):
        ahead = [scores(slot, 0), scores(slot, 1)] if diag else [sbuf[0], sbuf[1]]
        norm(j + 1)
        project(1 - slot)
        for p in range(pairs):
            now = ahead
            ahead = [scores(slot, 2 * p + 2 + i) if p + 1 < pairs else scores(1 - slot, i) for i in range(2)]
            vt = vst[slot, :, p * 2 * hd:(p + 1) * 2 * hd].T
            for i in range(2):
                h = 2 * p + i
                s = now[i]
                rows = slice(h * hd, (h + 1) * hd)
                vh = head_rows(vt, i, hd, False)
                if diag:
                    s = jnp.where(causal(T, True), s, NEG_BIG)
                    m = jnp.max(s, axis=0, keepdims=True)
                    e = jnp.exp(s - m)
                    lrow[h:h + 1] = jnp.sum(e, axis=0, keepdims=True)
                    acc[rows] = mm(vh, e.astype(jnp.bfloat16))
                else:
                    m_old = mrow[h:h + 1]
                    m = jnp.maximum(m_old, jnp.max(s, axis=0, keepdims=True))
                    e = jnp.exp(s - m)
                    alpha = jnp.exp(m_old - m)
                    lrow[h:h + 1] = lrow[h:h + 1] * alpha + jnp.sum(e, axis=0, keepdims=True)
                    acc[rows] = acc[rows] * alpha + mm(vh, e.astype(jnp.bfloat16))
                mrow[h:h + 1] = m
        sbuf[0], sbuf[1] = ahead

    for j in range(-1, DEEP - 1):
        start(fetch(jnp.int32(j)))
    own = jnp.int32(-1)
    wait(fetch(own))
    norm(own)
    project(0)
    for t in range(tiles):
        cols = slice(t * 256, (t + 1) * 256)
        q = rotate(mm(hsc[...], wq_ref[:, cols]) + b_ref[0:1, cols], cs[...], ss[...])
        qt_ref[cols] = (q.astype(jnp.bfloat16) * jnp.bfloat16(scale)).T
    put_masked(qtm, qt_ref[...], hd, True)
    start(flush(me, 0))
    start(fetch(own + DEEP))
    wait(fetch(own + 1))
    attend(own, 0, True)

    @pl.when(me >= 1)
    def _():
        start(flush(0, 1))

    wait(flush(me, 0))

    def step(j, slot):
        wait(fetch(j + 1))
        start(fetch(j + DEEP))

        @pl.when(j >= 1)
        def _():
            wait(flush(j - 1, 1 - slot))

        attend(j, slot, False)

        @pl.when(j + 1 < me)
        def _():
            start(flush(j + 1, 1 - slot))

        return 1 - slot

    last = lax.fori_loop(0, me, step, jnp.int32(1))

    for k in range(1, DEEP):
        wait(fetch(me + k))

    @pl.when(me >= 1)
    def _():
        wait(flush(me - 1, 1 - last))

    lse_ref[...] = mrow[...] + jnp.log(lrow[...])
    inv = 1.0 / lrow[...]
    for p in range(pairs):
        a = acc[2 * p * hd:(2 * p + 1) * hd] * inv[2 * p:2 * p + 1]
        b = acc[(2 * p + 1) * hd:(2 * p + 2) * hd] * inv[2 * p + 1:2 * p + 2]
        ctx_ref[:, 2 * p * hd:(2 * p + 2) * hd] = jnp.concatenate([a, b], axis=0).T


def fwd_attention(me, x_all, tab, gain, shift, wq, wk, wv, b3, T, hd):
    S, W = x_all.shape
    heads = W // hd
    vm = pl.BlockSpec(memory_space=pltpu.VMEM)
    anym = pl.BlockSpec(memory_space=pl.ANY)
    f32, bf = jnp.float32, jnp.bfloat16
    return pl.pallas_call(
        functools.partial(fwd_kernel, hd),
        out_shape=[jax.ShapeDtypeStruct((S, W), bf), jax.ShapeDtypeStruct((S, W), bf), jax.ShapeDtypeStruct((T, W), f32),
                   jax.ShapeDtypeStruct((heads, T), f32), jax.ShapeDtypeStruct((W, T), bf)],
        in_specs=[pl.BlockSpec(memory_space=pltpu.SMEM), anym] + [vm] * 10,
        out_specs=[anym, anym, vm, vm, vm],
        scratch_shapes=[pltpu.VMEM((4, T, W), bf), pltpu.VMEM((T, 128), f32), pltpu.VMEM((T, 128), f32), pltpu.VMEM((T, W), bf),
                        pltpu.VMEM((2, T, W), bf), pltpu.VMEM((2, T, W), bf), pltpu.VMEM((heads, 2 * hd, T), bf), pltpu.VMEM((2, T, T), f32),
                        pltpu.VMEM((W, T), f32), pltpu.VMEM((heads, T), f32), pltpu.VMEM((heads, T), f32),
                        pltpu.SemaphoreType.DMA((4,)), pltpu.SemaphoreType.DMA((2, 2))],
        compiler_params=pltpu.CompilerParams(vmem_limit_bytes=VMEM_LIMIT),
        cost_estimate=pl.CostEstimate(flops=40_000_000_000, bytes_accessed=40_000_000, transcendentals=0),
        name="attn_fwd",
    )(me, x_all, *tab, gain, shift, wq, wk, wv, b3)


def proj_kernel(hd, n, me_ref, x_hbm, dy_hbm, cl_ref, sl_ref, cb_ref, sb_ref, g_ref, s_ref, wq_ref, wot_ref, bq_ref, q_hbm, o_hbm,
                xb, yb, cs, ss, hsc, qst, ost, in_sem, out_sem):
    me = me_ref[0]
    DEEP, T, W = xb.shape
    scale = hd ** -0.5
    tab = (cl_ref, sl_ref, cb_ref, sb_ref)

    def fetch(r):
        slot, blk = r % DEEP, jnp.minimum(me + r, n - 1)
        return (pltpu.make_async_copy(x_hbm.at[pl.ds(blk * T, T)], xb.at[slot], in_sem.at[slot, 0]),
                pltpu.make_async_copy(dy_hbm.at[pl.ds(blk * T, T)], yb.at[slot], in_sem.at[slot, 1]))

    def flush(r):
        slot = r % 2
        return (pltpu.make_async_copy(qst.at[slot], q_hbm.at[pl.ds((me + r) * T, T)], out_sem.at[slot, 0]),
                pltpu.make_async_copy(ost.at[slot], o_hbm.at[pl.ds((me + r) * T, T)], out_sem.at[slot, 1]))

    def start(copies):
        for c in copies:
            c.start()

    def wait(copies):
        for c in copies:
            c.wait()

    for r in range(DEEP - 1):
        start(fetch(jnp.int32(r)))

    def step(r, _):
        start(fetch(r + DEEP - 1))
        wait(fetch(r))

        @pl.when(r >= 2)
        def _():
            wait(flush(r - 2))

        turn(tab, me + r, cs, ss)
        for t in range(W // 256):
            cols = slice(t * 256, (t + 1) * 256)
            ost[r % 2, :, cols] = mm(yb[r % DEEP], wot_ref[:, cols]).astype(jnp.bfloat16)
        hsc[...] = layer_norm(xb[r % DEEP].astype(jnp.float32), g_ref[...], s_ref[...])[0].astype(jnp.bfloat16)
        for t in range(W // 256):
            cols = slice(t * 256, (t + 1) * 256)
            q = rotate(mm(hsc[...], wq_ref[:, cols]) + bq_ref[:, cols], cs[...], ss[...])
            qst[r % 2, :, cols] = q.astype(jnp.bfloat16) * jnp.bfloat16(scale)
        start(flush(r))
        return 0

    count = n - me
    lax.fori_loop(0, count, step, 0)
    for k in range(DEEP - 1):
        wait(fetch(count + k))
    wait(flush(count - 1))

    @pl.when(count >= 2)
    def _():
        wait(flush(count - 2))


def later_blocks(me, x_all, dy_all, tab, gain, shift, wq, wot, bq, T, hd):
    S, W = x_all.shape
    vm = pl.BlockSpec(memory_space=pltpu.VMEM)
    anym = pl.BlockSpec(memory_space=pl.ANY)
    f32, bf = jnp.float32, jnp.bfloat16
    return pl.pallas_call(
        functools.partial(proj_kernel, hd, S // T),
        out_shape=[jax.ShapeDtypeStruct((S, W), bf)] * 2,
        in_specs=[pl.BlockSpec(memory_space=pltpu.SMEM), anym, anym] + [vm] * 9,
        out_specs=[anym, anym],
        scratch_shapes=[pltpu.VMEM((4, T, W), bf), pltpu.VMEM((4, T, W), bf), pltpu.VMEM((T, 128), f32), pltpu.VMEM((T, 128), f32), pltpu.VMEM((T, W), bf),
                        pltpu.VMEM((2, T, W), bf), pltpu.VMEM((2, T, W), bf), pltpu.SemaphoreType.DMA((4, 2)), pltpu.SemaphoreType.DMA((2, 2))],
        compiler_params=pltpu.CompilerParams(vmem_limit_bytes=VMEM_LIMIT),
        cost_estimate=pl.CostEstimate(flops=20_000_000_000, bytes_accessed=40_000_000, transcendentals=0),
        name="later_blocks",
    )(me, x_all, dy_all, *tab, gain, shift, wq, wot, bq)


def bwd_kernel(hd, n, srows, me_ref, k_hbm, v_hbm, q_hbm, o_hbm, stats_ref, qt_ref, own_ref, ct_ref, st_ref, d3_ref,
               kb, vb, qb, ob, am, bm, sbuf, acc1, acc2, kv_sem, qo_sem):
    me = me_ref[0]
    DEEP, T, W = kb.shape
    heads = W // hd
    half = hd // 8
    scale = hd ** -0.5

    def fetch_kv(j):
        slot, blk = j % DEEP, jnp.minimum(j, me)
        return (pltpu.make_async_copy(k_hbm.at[pl.ds(blk * T, T)], kb.at[slot], kv_sem.at[slot, 0]),
                pltpu.make_async_copy(v_hbm.at[pl.ds(blk * T, T)], vb.at[slot], kv_sem.at[slot, 1]))

    def fetch_qo(r):
        slot, blk = r % DEEP, jnp.minimum(me + r, n - 1)
        return (pltpu.make_async_copy(q_hbm.at[pl.ds(blk * T, T)], qb.at[slot], qo_sem.at[slot, 0]),
                pltpu.make_async_copy(o_hbm.at[pl.ds(blk * T, T)], ob.at[slot], qo_sem.at[slot, 1]))

    def start(copies):
        for c in copies:
            c.start()

    def wait(copies):
        for c in copies:
            c.wait()

    def pair_cols(h):
        return slice(h // 2 * 2 * hd, (h // 2 + 1) * 2 * hd)

    def unrotated(z):
        mid = hd // 2
        a, b = z[:half], z[mid:mid + half]
        ct, st = ct_ref[...], st_ref[...]
        return jnp.concatenate([a * ct + b * st, b * ct - a * st, z[half:mid], z[mid + half:]], axis=0)

    def two_scores(left, right, slot, h):
        return mm(left[slot, :, pair_cols(h)], am[h]), mm(right[slot, :, pair_cols(h)], bm[h])

    for r in range(DEEP - 1):
        start(fetch_kv(jnp.int32(r)))
        start(fetch_qo(jnp.int32(r)))
    put_masked(am, qt_ref[...], hd, True)
    put_masked(bm, own_ref[...].T, hd, False)
    acc1[...] = jnp.zeros_like(acc1)
    zero = jnp.int32(0)

    def dq_block(j, diag):
        slot = j % DEEP
        ahead = [(sbuf[0], sbuf[1]), (sbuf[2], sbuf[3])]
        for h in range(heads):
            s, dp = ahead.pop(0)
            ahead.append(two_scores(kb, vb, slot, h + 2) if h + 2 < heads else two_scores(kb, vb, (j + 1) % DEEP, h + 2 - heads))
            if h % 2 == 0:
                kt = kb[slot, :, pair_cols(h)].T
            if diag:
                s = jnp.where(causal(T, True), s, NEG_BIG)
            pr = jnp.exp(s - stats_ref[pl.ds(me * srows + h, 1), :])
            ds = (pr * (dp - stats_ref[pl.ds(me * srows + heads + h, 1), :])).astype(jnp.bfloat16)
            acc1[h * hd:(h + 1) * hd] += mm(head_rows(kt, h % 2, hd, True), ds)
        (sbuf[0], sbuf[1]), (sbuf[2], sbuf[3]) = ahead

    wait(fetch_kv(zero))
    sbuf[0], sbuf[1] = two_scores(kb, vb, 0, 0)
    sbuf[2], sbuf[3] = two_scores(kb, vb, 0, 1)

    def dq_step(j, _):
        start(fetch_kv(j + DEEP - 1))
        wait(fetch_kv(j + 1))
        dq_block(j, False)
        return 0

    lax.fori_loop(0, me, dq_step, 0)
    for k in range(1, DEEP - 1):
        wait(fetch_kv(me + k))
    dq_block(me, True)
    last = me % DEEP
    for h in range(heads):
        d3_ref[3 * h * hd:(3 * h + 1) * hd] = unrotated(acc1[h * hd:(h + 1) * hd] * scale)

    put_masked(am, kb[last].T, hd, True)
    put_masked(bm, vb[last].T, hd, False)
    acc1[...] = jnp.zeros_like(acc1)
    acc2[...] = jnp.zeros_like(acc2)

    def dkv_block(r, diag):
        slot = r % DEEP
        ahead = [(sbuf[0], sbuf[1]), (sbuf[2], sbuf[3])]
        stc = stats_ref[pl.ds((me + r) * srows, 2 * heads), :].T
        for h in range(heads):
            s, dp = ahead.pop(0)
            ahead.append(two_scores(qb, ob, slot, h + 2) if h + 2 < heads else two_scores(qb, ob, (r + 1) % DEEP, h + 2 - heads))
            if h % 2 == 0:
                qt = qb[slot, :, pair_cols(h)].T
                ot = ob[slot, :, pair_cols(h)].T
            if diag:
                s = jnp.where(causal(T, False), s, NEG_BIG)
            rows = slice(h * hd, (h + 1) * hd)
            pr = jnp.exp(s - stc[:, h:h + 1])
            acc2[rows] += mm(head_rows(ot, h % 2, hd, False), pr.astype(jnp.bfloat16))
            ds = (pr * (dp - stc[:, heads + h:heads + h + 1])).astype(jnp.bfloat16)
            acc1[rows] += mm(head_rows(qt, h % 2, hd, True), ds)
        (sbuf[0], sbuf[1]), (sbuf[2], sbuf[3]) = ahead

    wait(fetch_qo(zero))
    sbuf[0], sbuf[1] = two_scores(qb, ob, 0, 0)
    sbuf[2], sbuf[3] = two_scores(qb, ob, 0, 1)

    def dkv_step(r, diag):
        start(fetch_qo(r + DEEP - 1))
        wait(fetch_qo(r + 1))
        dkv_block(r, diag)
        return 0

    dkv_step(zero, True)
    lax.fori_loop(1, n - me, lambda r, _: dkv_step(r, False), 0)
    for k in range(1, DEEP - 1):
        wait(fetch_qo(n - me + k))
    for h in range(heads):
        d3_ref[(3 * h + 1) * hd:(3 * h + 2) * hd] = unrotated(acc1[h * hd:(h + 1) * hd])
        d3_ref[(3 * h + 2) * hd:(3 * h + 3) * hd] = acc2[h * hd:(h + 1) * hd]


def bwd_attention(me, k_all, v_all, q_all, o_all, stats, qt, d_ctx_bf, cos_t, sin_t, T, hd):
    S, W = k_all.shape
    heads = W // hd
    vm = pl.BlockSpec(memory_space=pltpu.VMEM)
    anym = pl.BlockSpec(memory_space=pl.ANY)
    f32, bf = jnp.float32, jnp.bfloat16
    return pl.pallas_call(
        functools.partial(bwd_kernel, hd, S // T, stats.shape[0] * T // S),
        out_shape=jax.ShapeDtypeStruct((3 * W, T), f32),
        in_specs=[pl.BlockSpec(memory_space=pltpu.SMEM)] + [anym] * 4 + [vm] * 5,
        out_specs=vm,
        scratch_shapes=[pltpu.VMEM((4, T, W), bf)] * 4 + [pltpu.VMEM((heads, 2 * hd, T), bf), pltpu.VMEM((heads, 2 * hd, T), bf),
                        pltpu.VMEM((4, T, T), f32), pltpu.VMEM((W, T), f32), pltpu.VMEM((W, T), f32),
                        pltpu.SemaphoreType.DMA((4, 2)), pltpu.SemaphoreType.DMA((4, 2))],
        compiler_params=pltpu.CompilerParams(vmem_limit_bytes=VMEM_LIMIT),
        cost_estimate=pl.CostEstimate(flops=100_000_000_000, bytes_accessed=30_000_000, transcendentals=0),
        name="attn_bwd",
    )(me, k_all, v_all, q_all, o_all, stats, qt, d_ctx_bf, cos_t, sin_t)


def mlp_kernel(x_ref, dy_ref, g_ref, s_ref, wu_ref, bu_ref, wd_ref, du_ref, db_ref):
    @pl.when(pl.program_id(0) == 0)
    def _():
        du_ref[...] = jnp.zeros_like(du_ref)
        db_ref[...] = jnp.zeros_like(db_ref)

    h = layer_norm(x_ref[...].astype(jnp.float32), g_ref[...], s_ref[...])[0].astype(jnp.bfloat16)
    dy = dy_ref[...]
    act, slope = exact_gelu(mm(h, wu_ref[...]) + bu_ref[...])
    d_up = mm(dy, wd_ref[...]) * slope
    keep = du_ref.shape[0] // 2
    db_ref[...] += jnp.sum(d_up, axis=0, keepdims=True)
    du_ref[:keep] += mm(d_up.astype(jnp.bfloat16).T, h)[:keep]
    du_ref[keep:] += mm(act.astype(jnp.bfloat16).T, dy)[:keep]


def mlp_grads(x_all, dy_all, gain, shift, wu, bu, wd, keep):
    S, W = x_all.shape
    F = wu.shape[1]
    R = 256
    const = lambda j: (0, 0)
    return pl.pallas_call(
        mlp_kernel,
        grid=(S // R,),
        out_shape=[jax.ShapeDtypeStruct((2 * keep, W), jnp.float32)] + [jax.ShapeDtypeStruct((1, F), jnp.float32)],
        in_specs=[pl.BlockSpec((R, W), lambda j: (j, 0)), pl.BlockSpec((R, W), lambda j: (j, 0)), pl.BlockSpec((1, W), const), pl.BlockSpec((1, W), const),
                  pl.BlockSpec((W, F), const), pl.BlockSpec((1, F), const), pl.BlockSpec((W, F), const)],
        out_specs=[pl.BlockSpec((2 * keep, W), const)] + [pl.BlockSpec((1, F), const)],
        compiler_params=pltpu.CompilerParams(vmem_limit_bytes=VMEM_LIMIT, dimension_semantics=("arbitrary",)),
        cost_estimate=pl.CostEstimate(flops=20_000_000_000, bytes_accessed=26_000_000, transcendentals=0),
        name="mlp_grads",
    )(x_all, dy_all, gain, shift, wu, bu, wd)


def solution(mesh):
    cp_size = mesh.shape['cp']
    row_spec = P('dp', 'cp', None)
    in_specs = (row_spec, row_spec) + (P(),) * 12
    out_specs = (row_spec, row_spec, P('dp'), P('dp'), P('dp'), P('dp'), P('dp', None, None, None), P('dp', None, None), P('dp', None), P('dp'), P('dp', None), P('dp'), P('dp', None), P('dp'))
    bf, f32 = jnp.bfloat16, jnp.float32

    def local_layer(x_blk, dy_blk, ln1_gain, ln1_bias, ln2_gain, ln2_bias, w_qkv, b_qkv, w_out, b_out, w_up, b_up, w_down, b_down):
        T, W = x_blk.shape[1:]
        heads, hd = w_qkv.shape[1], w_qkv.shape[3]
        FF = w_up.shape[1]
        S = T * cp_size
        me = lax.axis_index('cp')
        me1 = me.astype(jnp.int32).reshape(1)
        row = lambda v: v.reshape(1, -1).astype(f32)

        TN = (((0,), (0,)), ((), ()))
        x_own = x_blk[0]
        dy_own = dy_blk[0]
        dy_bf = dy_own.astype(bf)
        x_all = lax.all_gather(x_own, 'cp', tiled=True)
        dy_all = lax.all_gather(dy_bf, 'cp', tiled=True)

        w_rows = w_qkv.transpose(1, 2, 3, 0)
        wq, wk = (pair_rows(w_rows[:, c]).T for c in (0, 1))
        wv = w_rows[:, 2].reshape(W, W).T
        b_rows = b_qkv.astype(f32)[..., None]
        b3 = jnp.stack([pair_rows(b_rows[:, 0])[:, 0], pair_rows(b_rows[:, 1])[:, 0], b_rows[:, 2].reshape(W)])
        wot = w_out.T
        tab = lane_tables(jnp.arange(T), hd) + lane_tables(jnp.arange(cp_size) * T, hd)
        ang = rope_angles(me * T + jnp.arange(T), hd).T
        cos_o, sin_o = jnp.cos(ang), jnp.sin(ang)

        x_rows = x_own.astype(f32)
        h_attn, x_norm1, inv_std1 = layer_norm(x_rows, ln1_gain, ln1_bias)
        h_attn = h_attn.astype(bf)
        h_mlp, x_norm2, inv_std2 = layer_norm(x_rows, ln2_gain, ln2_bias)
        h_mlp = h_mlp.astype(bf)
        gelu_out, slope = exact_gelu(mm(h_mlp, w_up) + b_up.astype(f32))
        y_part = x_rows + (mm(gelu_out.astype(bf), w_down) + b_down.astype(f32)) + b_out.astype(f32)
        d_up_bf = (mm(dy_bf, w_down, NT) * slope).astype(bf)
        d_h_mlp = mm(d_up_bf, w_up, NT)
        d_ctx = mm(dy_bf, w_out, NT)
        d_ctx_bf = d_ctx.astype(bf)
        dx_mlp, d_ln2_gain, d_ln2_bias = norm_backward(d_h_mlp, x_norm2, inv_std2, ln2_gain)
        dx_part = dy_own + dx_mlp
        dy_sum = jnp.sum(dy_own, axis=0)
        F = FF // cp_size
        F_pad = -(-F // 128) * 128
        pad = lambda a, ax: jnp.pad(a, [(0, F_pad - F) if d == ax else (0, 0) for d in range(a.ndim)])
        wu_s = pad(lax.dynamic_slice_in_dim(w_up, me * F, F, 1), 1)
        bu_s = pad(lax.dynamic_slice_in_dim(b_up.astype(f32), me * F, F, 0), 0).reshape(1, F_pad)
        wd_s = pad(lax.dynamic_slice_in_dim(w_down, me * F, F, 0).T, 1)

        (x_in, y_part, dx_part, d_ln2_gain, d_ln2_bias, dy_sum, d_ctx, d_ctx_bf, h_attn, wq, wk, wv, wot, wu_s, wd_s) = lax.optimization_barrier(
            (x_all, y_part, dx_part, d_ln2_gain, d_ln2_bias, dy_sum, d_ctx, d_ctx_bf, h_attn, wq, wk, wv, wot, wu_s, wd_s))
        k_all, v_all, attn_norm, lse, qt = fwd_attention(me1, x_in, tab, row(ln1_gain), row(ln1_bias), wq, wk, wv, b3, T, hd)
        delta = jnp.sum((d_ctx * attn_norm).reshape(T, heads, hd), axis=-1).T
        fill = jnp.zeros((-2 * heads % 32, T), f32)
        stats = lax.all_gather(jnp.concatenate([lse, delta, fill], axis=0), 'cp', tiled=True)
        attn_ctx = attn_norm.astype(bf)
        y_rows = (y_part + mm(attn_ctx, w_out)).astype(bf)
        d_w_out = mm(attn_ctx, dy_bf, TN)

        dy_in, _ = lax.optimization_barrier((dy_all, lse))
        du_s, db_s = mlp_grads(x_in, dy_in, row(ln2_gain), row(ln2_bias), wu_s, bu_s, wd_s, F)
        d_b_up = lax.dynamic_update_slice(jnp.zeros((FF,), f32), db_s[0, :F], (me * F,))

        dy_late, _ = lax.optimization_barrier((dy_in, db_s))
        q_all, o_all = later_blocks(me1, x_in, dy_late, tab, row(ln1_gain), row(ln1_bias), wq, wot, b3[0:1], T, hd)
        stats, d_w_out, q_all = lax.optimization_barrier((stats, d_w_out, q_all))
        d_w_mlp = lax.all_gather(du_s, 'cp', tiled=True)
        d3 = bwd_attention(me1, k_all, v_all, q_all, o_all, stats, qt, d_ctx_bf, cos_o, sin_o, T, hd)
        d3, d_w_mlp = lax.optimization_barrier((d3, d_w_mlp))
        d_w_mlp = d_w_mlp.reshape(cp_size, 2, F, W)
        d_w_up, d_w_down = d_w_mlp[:, 0].reshape(FF, W), d_w_mlp[:, 1].reshape(FF, W)
        d3_bf = d3.astype(bf)
        d_h = mm(d3_bf, w_rows.reshape(3 * W, W), TN)
        d_w_rows = mm(d3_bf, h_attn)
        dx_attn, d_ln1_gain, d_ln1_bias = norm_backward(d_h, x_norm1, inv_std1, ln1_gain)
        dx_rows = dx_part + dx_attn
        small = jnp.concatenate([d_ln1_gain, d_ln1_bias, d_ln2_gain, d_ln2_bias, dy_sum, jnp.sum(d3, axis=1), d_b_up]).reshape(-1, W)
        d_w_rows, tail = lax.psum((d_w_rows, jnp.concatenate([d_w_out, small], axis=0)), 'cp')
        d_w_out = tail[:W]
        small = tail[W:].reshape(-1)
        d_w_qkv = d_w_rows.reshape(heads, 3, hd, W).transpose(3, 0, 1, 2)
        vec = [small[i * W:(i + 1) * W] for i in range(5)]
        d_b_qkv = small[5 * W:8 * W].reshape(heads, 3, hd)
        d_b_up = small[8 * W:]
        return (y_rows[None], dx_rows[None], vec[0], vec[1], vec[2], vec[3], d_w_qkv, d_b_qkv, d_w_out, vec[4], d_w_up.T, d_b_up, d_w_down, vec[4])

    return jax.shard_map(local_layer, mesh=mesh, in_specs=in_specs, out_specs=out_specs, check_vma=False)
```
